32 devices in a mesh: pod: 8 (over z, y), data: 4 (over x, core).
Axes of the slice: x: 2, y: 2, z: 4, core: 2. Of those that a mesh axis runs over, the one named last changes fastest.
Arguments:
- feat_a: bfloat16 [16384, 512], P(('pod', 'data'))
- feat_b: bfloat16 [16384, 512], P(('pod', 'data'))
- w_first: bfloat16 [512, 2048], replicated
- w_second: bfloat16 [2048, 2048], replicated
- w_third: bfloat16 [2048, 2048], replicated
- gain_first: float32 [2048], replicated
- shift_first: float32 [2048], replicated
- gain_second: float32 [2048], replicated
- shift_second: float32 [2048], replicated
- lam_off: float32 [], replicated
Outputs:
- output 1: float32 [], replicated
- output 2: float32 [512, 2048], replicated
- output 3: float32 [2048, 2048], replicated
- output 4: float32 [2048, 2048], replicated
- output 5: float32 [2048], replicated
- output 6: float32 [2048], replicated
- output 7: float32 [2048], replicated
- output 8: float32 [2048], replicated
All inputs are finite; a program needn't handle non-finite values.
Results may differ from the reference program's by a relative error of at most 0.001.
Values are sent between devices in bfloat16 or wider.
A program may use at most 1 GiB of HBM per device.

```python
import jax
import jax.numpy as jnp
from jax import lax

ROWS_DEV = 512
NUM_DEVICES = 32
FEAT_DIM = 512
PROJ_DIM = 2048
NUM_ROWS = ROWS_DEV * NUM_DEVICES
BN_EPS = 1e-5


def setup_inputs(seed: int = 0) -> dict:
    key_list = jax.random.split(jax.random.key(seed), 12)
    block_shape = (NUM_DEVICES, ROWS_DEV, FEAT_DIM)
    stat_shape = (NUM_DEVICES, 1, FEAT_DIM)
    base_vals = jax.random.normal(key_list[0], block_shape, jnp.float32)
    noise_vals = jax.random.normal(key_list[1], block_shape, jnp.float32)
    shard_shift = 0.7 * jax.random.normal(key_list[2], stat_shape, jnp.float32)
    shard_scale = jax.random.uniform(key_list[3], stat_shape, jnp.float32, 0.5, 1.5)
    view_a = base_vals * shard_scale + shard_shift
    view_b = (0.8 * base_vals + 0.6 * noise_vals) * shard_scale + shard_shift
    w_first = jax.random.normal(key_list[4], (FEAT_DIM, PROJ_DIM), jnp.float32) * FEAT_DIM ** -0.5
    w_second = jax.random.normal(key_list[5], (PROJ_DIM, PROJ_DIM), jnp.float32) * PROJ_DIM ** -0.5
    w_third = jax.random.normal(key_list[6], (PROJ_DIM, PROJ_DIM), jnp.float32) * PROJ_DIM ** -0.5
    lam_off = (0.05 + 0.1 * jax.random.uniform(key_list[11], (), jnp.float32)) * NUM_ROWS / PROJ_DIM
    return {
        'feat_a': view_a.reshape(NUM_ROWS, FEAT_DIM).astype(jnp.bfloat16),
        'feat_b': view_b.reshape(NUM_ROWS, FEAT_DIM).astype(jnp.bfloat16),
        'w_first': w_first.astype(jnp.bfloat16),
        'w_second': w_second.astype(jnp.bfloat16),
        'w_third': w_third.astype(jnp.bfloat16),
        'gain_first': 1.0 + 0.3 * jax.random.normal(key_list[7], (PROJ_DIM,), jnp.float32),
        'shift_first': 0.5 * jax.random.normal(key_list[8], (PROJ_DIM,), jnp.float32),
        'gain_second': 1.0 + 0.3 * jax.random.normal(key_list[9], (PROJ_DIM,), jnp.float32),
        'shift_second': 0.5 * jax.random.normal(key_list[10], (PROJ_DIM,), jnp.float32),
        'lam_off': lam_off,
    }


def batch_norm(pre_act):
    feat_mean = jnp.sum(pre_act, axis=0) / NUM_ROWS
    sq_mean = jnp.sum(pre_act * pre_act, axis=0) / NUM_ROWS
    inv_std = lax.rsqrt(sq_mean - feat_mean * feat_mean + BN_EPS)
    return (pre_act - feat_mean) * inv_std, inv_std


def project(feats_in, w_first, w_second, w_third, gain_first, shift_first, gain_second, shift_second):
    pre_one = jnp.dot(feats_in, w_first, preferred_element_type=jnp.float32)
    norm_one, inv_one = batch_norm(pre_one)
    post_one = gain_first * norm_one + shift_first
    hid_one = jnp.maximum(post_one, 0.0).astype(jnp.bfloat16)
    pre_two = jnp.dot(hid_one, w_second, preferred_element_type=jnp.float32)
    norm_two, inv_two = batch_norm(pre_two)
    post_two = gain_second * norm_two + shift_second
    hid_two = jnp.maximum(post_two, 0.0).astype(jnp.bfloat16)
    proj_out = jnp.dot(hid_two, w_third, preferred_element_type=jnp.float32)
    emb_norm, inv_three = batch_norm(proj_out)
    return (norm_one, inv_one, post_one, hid_one, norm_two, inv_two, post_two, hid_two, emb_norm, inv_three)


def norm_backward(grad_norm, normed, inv_std):
    grad_mean = jnp.sum(grad_norm, axis=0) / NUM_ROWS
    cross_mean = jnp.sum(grad_norm * normed, axis=0) / NUM_ROWS
    return inv_std * (grad_norm - grad_mean - normed * cross_mean)


def back_project(grad_emb, feats_in, saved, w_second, w_third, gain_first, gain_second):
    norm_one, inv_one, post_one, hid_one, norm_two, inv_two, post_two, hid_two, emb_norm, inv_three = saved
    grad_proj = norm_backward(grad_emb, emb_norm, inv_three).astype(jnp.bfloat16)
    grad_third = jnp.dot(hid_two.T, grad_proj, preferred_element_type=jnp.float32)
    grad_act_two = jnp.where(post_two > 0, jnp.dot(grad_proj, w_third.T, preferred_element_type=jnp.float32), 0.0)
    grad_gain_two = jnp.sum(grad_act_two * norm_two, axis=0)
    grad_shift_two = jnp.sum(grad_act_two, axis=0)
    grad_pre_two = norm_backward(gain_second * grad_act_two, norm_two, inv_two).astype(jnp.bfloat16)
    grad_second = jnp.dot(hid_one.T, grad_pre_two, preferred_element_type=jnp.float32)
    grad_act_one = jnp.where(post_one > 0, jnp.dot(grad_pre_two, w_second.T, preferred_element_type=jnp.float32), 0.0)
    grad_gain_one = jnp.sum(grad_act_one * norm_one, axis=0)
    grad_shift_one = jnp.sum(grad_act_one, axis=0)
    grad_pre_one = norm_backward(gain_first * grad_act_one, norm_one, inv_one).astype(jnp.bfloat16)
    grad_first = jnp.dot(feats_in.T, grad_pre_one, preferred_element_type=jnp.float32)
    return (grad_first, grad_second, grad_third, grad_gain_one, grad_shift_one, grad_gain_two, grad_shift_two)


def reference(feat_a, feat_b, w_first, w_second, w_third, gain_first, shift_first, gain_second, shift_second, lam_off):
    saved_a = project(feat_a, w_first, w_second, w_third, gain_first, shift_first, gain_second, shift_second)
    saved_b = project(feat_b, w_first, w_second, w_third, gain_first, shift_first, gain_second, shift_second)
    emb_a = saved_a[8].astype(jnp.bfloat16)
    emb_b = saved_b[8].astype(jnp.bfloat16)
    corr_mat = jnp.dot(emb_a.T, emb_b, preferred_element_type=jnp.float32) / NUM_ROWS
    on_diag = jnp.diagonal(corr_mat)
    total_loss = jnp.sum((1.0 - on_diag) ** 2) + lam_off * (jnp.sum(corr_mat * corr_mat) - jnp.sum(on_diag * on_diag))
    diag_mask = jnp.arange(PROJ_DIM)[:, None] == jnp.arange(PROJ_DIM)[None, :]
    grad_corr = jnp.where(diag_mask, -2.0 * (1.0 - corr_mat), 2.0 * lam_off * corr_mat).astype(jnp.bfloat16)
    grad_emb_a = jnp.dot(emb_b, grad_corr.T, preferred_element_type=jnp.float32) / NUM_ROWS
    grad_emb_b = jnp.dot(emb_a, grad_corr, preferred_element_type=jnp.float32) / NUM_ROWS
    grads_a = back_project(grad_emb_a, feat_a, saved_a, w_second, w_third, gain_first, gain_second)
    grads_b = back_project(grad_emb_b, feat_b, saved_b, w_second, w_third, gain_first, gain_second)
    return (total_loss, grads_a[0] + grads_b[0], grads_a[1] + grads_b[1], grads_a[2] + grads_b[2], grads_a[3] + grads_b[3], grads_a[4] + grads_b[4], grads_a[5] + grads_b[5], grads_a[6] + grads_b[6])
```

```python
import functools
import jax
import jax.numpy as jnp
from jax import lax
from jax.experimental import pallas as pl
from jax.experimental.pallas import tpu as pltpu
from jax.sharding import PartitionSpec as P

BN_EPS = 1e-5
ROW_AXES = ('pod', 'data')
MESH = pl.DeviceIdType.MESH
WIDTH = 2048
QCOLS = WIDTH // 4
CHUNK = 128
BLOCK = CHUNK // 2


def coordinates():
    pod, dat = lax.axis_index('pod'), lax.axis_index('data')
    return lax.div(pod, 2), lax.rem(pod, 2), lax.div(dat, 2), lax.rem(dat, 2)


def device(z, y, x, c):
    return (z * 2 + y, x * 2 + c)


def remote(src, dst, send, recv, dev):
    copy = pltpu.make_async_remote_copy(src_ref=src, dst_ref=dst, send_sem=send, recv_sem=recv, device_id=dev, device_id_type=MESH)
    copy.start()
    return copy


def meet(peers):
    barrier = pltpu.get_barrier_semaphore()
    for dev in peers:
        pl.semaphore_signal(barrier, inc=1, device_id=dev, device_id_type=MESH)
    pl.semaphore_wait(barrier, len(peers))


def stat_kernel(half, v_ref, o_ref, from_core, plane, line, send, recv):
    z, y, x, c = coordinates()
    core_peer = device(z, y, x, 1 - c)
    plane_peers = [device(z, y, 1 - x, c), device(z, 1 - y, x, c), device(z, 1 - y, 1 - x, c)]
    line_peers = [device(lax.rem(z + o, 4), y, x, c) for o in (1, 2, 3)]
    meet([core_peer] + plane_peers + line_peers)
    mine = pl.ds(pl.multiple_of(c * half, 128), half)
    theirs = pl.ds(pl.multiple_of((1 - c) * half, 128), half)
    copies = [remote(v_ref.at[:, theirs], from_core, send.at[0], recv.at[0], core_peer)]
    copies[0].wait_recv()
    spot = y * 2 + x
    plane[spot] = v_ref[:, mine] + from_core[...]
    for i, dev in enumerate(plane_peers):
        copies.append(remote(plane.at[spot], plane.at[spot], send.at[1 + i], recv.at[1 + i], dev))
    for copy in copies[1:4]:
        copy.wait_recv()
    line[z] = (plane[0] + plane[1]) + (plane[2] + plane[3])
    for i, dev in enumerate(line_peers):
        copies.append(remote(line.at[z], line.at[z], send.at[4 + i], recv.at[4 + i], dev))
    for copy in copies[4:7]:
        copy.wait_recv()
    o_ref[:, mine] = (line[0] + line[1]) + (line[2] + line[3])
    copies.append(remote(o_ref.at[:, mine], o_ref.at[:, mine], send.at[7], recv.at[7], core_peer))
    copies[7].wait_recv()
    for copy in copies:
        copy.wait_send()


def sum_stats(values, collective_id):
    rows, width = values.shape
    half = width // 2
    return pl.pallas_call(
        functools.partial(stat_kernel, half),
        out_shape=jax.ShapeDtypeStruct((rows, width), jnp.float32),
        in_specs=[pl.BlockSpec(memory_space=pltpu.VMEM)],
        out_specs=pl.BlockSpec(memory_space=pltpu.VMEM),
        scratch_shapes=[pltpu.VMEM((rows, half), jnp.float32), pltpu.VMEM((4, rows, half), jnp.float32), pltpu.VMEM((4, rows, half), jnp.float32),
                        pltpu.SemaphoreType.DMA((8,)), pltpu.SemaphoreType.DMA((8,))],
        compiler_params=pltpu.CompilerParams(collective_id=collective_id, has_side_effects=True),
    )(values)


def chunk_plan(row_counts, late):
    plan, counts = [], [0, 0]
    for a, rows in enumerate(row_counts):
        for k in range(rows // 2 // CHUNK):
            kind = 1 if len(plan) % late == late - 1 else 0
            plan.append((a, k, kind, counts[kind]))
            counts[kind] += 1
    return plan, counts


def reduce_kernel(row_counts, plan, num_rows, *refs):
    count = len(row_counts)
    make_grad = num_rows is not None
    parts, refs = refs[:count], refs[count:]
    if make_grad:
        lam_ref, refs = refs[0], refs[1:]
    outs, refs = refs[:count], refs[count:]
    if make_grad:
        loss_ref, refs = refs[0], refs[1:]
    own, from_core, recv_first, recv_rows, recv_line, send, recv, core_send, core_recv, local_sem = refs[:10]
    if make_grad:
        shard = refs[10]
    z, y, x, c = coordinates()
    core_peer = device(z, y, x, 1 - c)
    row_peer = {'x': device(z, y, 1 - x, c), 'y': device(z, 1 - y, x, c)}
    row_pos = {'x': x, 'y': y}
    line_peers = [device(lax.rem(z + o, 4), y, x, c) for o in (1, 2, 3)]
    meet([core_peer, row_peer['x'], row_peer['y']] + line_peers)
    chunks = len(plan)
    sends = []
    order = lambda kind, j: (('x', 'y', 'z'), ('y', 'x', 'z'))[j] if kind == 0 else (('x', 'z', 'y'), ('y', 'z', 'x'))[j]
    state = {}

    def start(k):
        a, n, kind, slot = plan[k]
        half = row_counts[a] // 2
        mine = pl.ds(pl.multiple_of(c * half + n * CHUNK, CHUNK), CHUNK)
        theirs = pl.ds(pl.multiple_of((1 - c) * half + n * CHUNK, CHUNK), CHUNK)
        load = pltpu.make_async_copy(parts[a].at[mine], own.at[k], local_sem.at[k, 2])
        load.start()
        copy = remote(parts[a].at[theirs], from_core.at[k], core_send.at[k, 0], core_recv.at[k, 0], core_peer)
        sends.append(copy)
        state[k] = {'load': load, 'core': copy}
        for j in range(2):
            state[k, j] = dict(row=j * BLOCK, rows=BLOCK, col=0, cols=WIDTH)

    def at(k, s):
        return (k, pl.ds(s['row'] if isinstance(s['row'], int) else pl.multiple_of(s['row'], 16), s['rows']),
                pl.ds(s['col'] if isinstance(s['col'], int) else pl.multiple_of(s['col'], QCOLS), s['cols']))

    def landing(k, j, dim, step):
        _, _, kind, slot = plan[k]
        if step == 0:
            return recv_first.at[k, j]
        if dim == 'z':
            return recv_line[kind].at[slot, j]
        return recv_rows[kind].at[slot, j]

    def scatter(k, j, step):
        dim = order(plan[k][2], j)[step]
        s = state[k, j]
        base = 0 if step == 0 else (1 if step == 1 else 2 if order(plan[k][2], j)[1] != 'z' else 4)
        copies = []
        if dim == 'z':
            for i, dev in enumerate(line_peers):
                part = dict(s, col=lax.rem(z + 1 + i, 4) * QCOLS, cols=QCOLS)
                copies.append(remote(own.at[at(k, part)], landing(k, j, dim, step).at[i], send.at[k, j, base + i], recv.at[k, j, base + i], dev))
            s.update(col=z * QCOLS, cols=QCOLS)
        else:
            half = s['rows'] // 2
            part = dict(s, row=s['row'] + (1 - row_pos[dim]) * half, rows=half)
            copies.append(remote(own.at[at(k, part)], landing(k, j, dim, step), send.at[k, j, base], recv.at[k, j, base], row_peer[dim]))
            s.update(row=s['row'] + row_pos[dim] * half, rows=half)
        sends.extend(copies)
        s['copies'] = copies
        s['land'] = landing(k, j, dim, step)

    def absorb(k, j):
        s = state[k, j]
        for copy in s['copies']:
            copy.wait_recv()
        if len(s['copies']) == 3:
            own[at(k, s)] = (own[at(k, s)] + s['land'][0]) + (s['land'][1] + s['land'][2])
        else:
            own[at(k, s)] = own[at(k, s)] + s['land'][...]

    def first(k):
        state[k]['load'].wait()
        state[k]['core'].wait_recv()
        own[k] = own[k] + from_core[k]
        for j in range(2):
            scatter(k, j, 0)

    def middle(step, k):
        for j in range(2):
            absorb(k, j)
            scatter(k, j, step)

    def out_at(k, s):
        a, n, _, _ = plan[k]
        row = c * (row_counts[a] // 2) + n * CHUNK + s['row']
        return outs[a].at[pl.ds(pl.multiple_of(row, 16), s['rows']), pl.ds(s['col'] if isinstance(s['col'], int) else pl.multiple_of(s['col'], QCOLS), s['cols'])]

    def gather(k, j, step):
        dim = order(plan[k][2], j)[2 - step]
        s = state[k, j]
        base = 5 + (0 if step == 0 else 4 if step == 2 else (1 if order(plan[k][2], j)[2] != 'z' else 3))
        src = out_at(k, s) if step else s['src']
        dst = out_at(k, s)
        copies = []
        if dim == 'z':
            for i, dev in enumerate(line_peers):
                copies.append(remote(src, dst, send.at[k, j, base + i], recv.at[k, j, base + i], dev))
            s.update(col=0, cols=WIDTH)
        else:
            copies.append(remote(src, dst, send.at[k, j, base], recv.at[k, j, base], row_peer[dim]))
            s.update(row=s['row'] - row_pos[dim] * s['rows'], rows=2 * s['rows'])
        sends.extend(copies)
        s['copies'] = copies

    def turn(k):
        a, n, _, _ = plan[k]
        for j in range(2):
            absorb(k, j)
            s = state[k, j]
            if make_grad:
                lam = lam_ref[0, 0]
                corr = own[at(k, s)] * (1.0 / num_rows)
                row = c * (row_counts[a] // 2) + n * CHUNK + s['row'] + lax.broadcasted_iota(jnp.int32, corr.shape, 0)
                col = s['col'] + lax.broadcasted_iota(jnp.int32, corr.shape, 1)
                diag = row == col
                miss = 1.0 - corr
                loss = jnp.where(diag, miss * miss, lam * (corr * corr))
                loss_ref[...] = loss if (k == 0 and j == 0) else loss_ref[...] + loss
                shard[k, j] = jnp.where(diag, -2.0 * miss, (2.0 * lam) * corr).astype(jnp.bfloat16)
                s['src'] = shard.at[k, j]
            else:
                s['src'] = own.at[at(k, s)]
            keep = pltpu.make_async_copy(s['src'], out_at(k, s), local_sem.at[k, j])
            keep.start()
            s['keep'] = keep
            gather(k, j, 0)

    def spread(step, k):
        for j in range(2):
            s = state[k, j]
            for copy in s['copies']:
                copy.wait_recv()
            if step == 1:
                s['keep'].wait()
            gather(k, j, step)

    def pair(k):
        a, n, _, _ = plan[k]
        for j in range(2):
            for copy in state[k, j]['copies']:
                copy.wait_recv()
        row = pl.ds(pl.multiple_of(c * (row_counts[a] // 2) + n * CHUNK, CHUNK), CHUNK)
        copy = remote(outs[a].at[row], outs[a].at[row], core_send.at[k, 1], core_recv.at[k, 1], core_peer)
        sends.append(copy)
        state[k]['pair'] = copy

    for k in range(chunks):
        start(k)
    stages = [first, functools.partial(middle, 1), functools.partial(middle, 2), turn, functools.partial(spread, 1), functools.partial(spread, 2), pair]
    for t in range(chunks + len(stages) - 1):
        for i, stage in enumerate(stages):
            if 0 <= t - i < chunks:
                stage(t - i)
    for k in range(chunks):
        state[k]['pair'].wait_recv()
    for copy in sends:
        copy.wait_send()


def reduce_all(parts, collective_id, lam=None, num_rows=None, late=3):
    row_counts = [p.shape[0] for p in parts]
    plan, counts = chunk_plan(row_counts, late)
    chunks = len(plan)
    any_spec = pl.BlockSpec(memory_space=pl.ANY)
    make_grad = lam is not None
    out_type = jnp.bfloat16 if make_grad else jnp.float32
    in_specs = [any_spec] * len(parts)
    out_specs = [any_spec] * len(parts)
    out_shape = [jax.ShapeDtypeStruct(p.shape, out_type) for p in parts]
    args = list(parts)
    if make_grad:
        in_specs.append(pl.BlockSpec(memory_space=pltpu.SMEM))
        args.append(lam.reshape(1, 1))
        out_specs.append(pl.BlockSpec(memory_space=pltpu.VMEM))
        out_shape.append(jax.ShapeDtypeStruct((BLOCK // 4, QCOLS), jnp.float32))
    ab, ef = counts
    f32 = jnp.float32
    scratch = [
        pltpu.VMEM((chunks, CHUNK, WIDTH), f32),
        pltpu.VMEM((chunks, CHUNK, WIDTH), f32),
        pltpu.VMEM((chunks, 2, BLOCK // 2, WIDTH), f32),
        [pltpu.VMEM((ab, 2, BLOCK // 4, WIDTH), f32), pltpu.VMEM((ef, 2, BLOCK // 4, QCOLS), f32)],
        [pltpu.VMEM((ab, 2, 3, BLOCK // 4, QCOLS), f32), pltpu.VMEM((ef, 2, 3, BLOCK // 2, QCOLS), f32)],
        pltpu.SemaphoreType.DMA((chunks, 2, 10)), pltpu.SemaphoreType.DMA((chunks, 2, 10)),
        pltpu.SemaphoreType.DMA((chunks, 2)), pltpu.SemaphoreType.DMA((chunks, 2)), pltpu.SemaphoreType.DMA((chunks, 3)),
    ]
    if make_grad:
        scratch.append(pltpu.VMEM((chunks, 2, BLOCK // 4, QCOLS), jnp.bfloat16))
    return pl.pallas_call(
        functools.partial(reduce_kernel, row_counts, plan, num_rows if make_grad else None),
        out_shape=out_shape, in_specs=in_specs, out_specs=out_specs, scratch_shapes=scratch,
        compiler_params=pltpu.CompilerParams(collective_id=collective_id, has_side_effects=True, vmem_limit_bytes=56 * 1024 * 1024),
    )(*args)


def total_stats(first, second, collective_id):
    local = jnp.concatenate([first, second])
    return sum_stats(local, collective_id).reshape(2, 2, WIDTH)


def batch_norm(pre_act, num_rows):
    totals = total_stats(jnp.sum(pre_act, axis=1), jnp.sum(pre_act * pre_act, axis=1), 0) / num_rows
    inv_std = lax.rsqrt(totals[1] - totals[0] * totals[0] + BN_EPS)[:, None, :]
    return (pre_act - totals[0][:, None, :]) * inv_std, inv_std


def run_layer(hidden, weight, gain_vec, shift_vec, num_rows):
    pre_act = jnp.einsum('vnf,fd->vnd', hidden, weight, preferred_element_type=jnp.float32)
    normed, inv_std = batch_norm(pre_act, num_rows)
    post_affine = gain_vec * normed + shift_vec
    return jnp.maximum(post_affine, 0.0).astype(jnp.bfloat16), post_affine, normed, inv_std


def affine_backward(grad_hid, post_affine, normed, inv_std, gain_vec, num_rows):
    grad_act = jnp.where(post_affine > 0, grad_hid, 0.0)
    totals = total_stats(jnp.sum(grad_act * normed, axis=1), jnp.sum(grad_act, axis=1), 0)
    grad_pre = (gain_vec * inv_std) * (grad_act - totals[1][:, None, :] / num_rows - normed * (totals[0][:, None, :] / num_rows))
    return grad_pre.astype(jnp.bfloat16), jnp.sum(totals[0], axis=0), jnp.sum(totals[1], axis=0)


def device_step(num_dev, feat_a, feat_b, w_first, w_second, w_third, gain_first, shift_first, gain_second, shift_second, lam_off):
    num_rows = feat_a.shape[0] * num_dev
    both_views = jnp.stack([feat_a, feat_b])
    hid_one, post_one, norm_one, inv_one = run_layer(both_views, w_first, gain_first, shift_first, num_rows)
    hid_two, post_two, norm_two, inv_two = run_layer(hid_one, w_second, gain_second, shift_second, num_rows)
    proj_out = jnp.einsum('vnf,fd->vnd', hid_two, w_third, preferred_element_type=jnp.float32)
    emb_norm, inv_three = batch_norm(proj_out, num_rows)
    emb_bf = emb_norm.astype(jnp.bfloat16)
    corr_part = lax.dot_general(emb_bf[0], emb_bf[1], (((0,), (0,)), ((), ())), preferred_element_type=jnp.float32)
    grad_corr, loss_part = reduce_all([corr_part], 2, lam_off, num_rows)
    grad_emb_a = lax.dot_general(emb_bf[1], grad_corr, (((1,), (1,)), ((), ())), preferred_element_type=jnp.float32)
    grad_emb_b = jnp.dot(emb_bf[0], grad_corr, preferred_element_type=jnp.float32)
    grad_emb = jnp.stack([grad_emb_a, grad_emb_b]) / num_rows
    local = jnp.concatenate([jnp.sum(grad_emb, axis=1), jnp.sum(grad_emb * emb_norm, axis=1)])
    extra = jnp.full((4, 256), jnp.sum(loss_part), jnp.float32)
    totals = sum_stats(jnp.concatenate([local, extra], axis=1), 1)
    total_loss = totals[0, WIDTH]
    totals = totals[:, :WIDTH].reshape(2, 2, WIDTH) / num_rows
    grad_proj = (inv_three * (grad_emb - totals[0][:, None, :] - emb_norm * totals[1][:, None, :])).astype(jnp.bfloat16)
    grad_third = jnp.einsum('woe,wof->ef', hid_two, grad_proj, preferred_element_type=jnp.float32)
    grad_hid_two = jnp.einsum('wof,ef->woe', grad_proj, w_third, preferred_element_type=jnp.float32)
    grad_pre_two, grad_gain_second, grad_shift_second = affine_backward(grad_hid_two, post_two, norm_two, inv_two, gain_second, num_rows)
    grad_second = jnp.einsum('woe,wof->ef', hid_one, grad_pre_two, preferred_element_type=jnp.float32)
    grad_hid_one = jnp.einsum('wof,ef->woe', grad_pre_two, w_second, preferred_element_type=jnp.float32)
    grad_pre_one, grad_gain_first, grad_shift_first = affine_backward(grad_hid_one, post_one, norm_one, inv_one, gain_first, num_rows)
    grad_first = jnp.einsum('vnf,vnd->fd', both_views, grad_pre_one, preferred_element_type=jnp.float32)
    (grad_third,) = reduce_all([grad_third], 3)
    grad_second, grad_first = reduce_all([grad_second, grad_first], 4)
    return (total_loss, grad_first, grad_second, grad_third, grad_gain_first, grad_shift_first, grad_gain_second, grad_shift_second)


def solution(mesh):
    num_dev = mesh.shape['pod'] * mesh.shape['data']
    row_spec = P(ROW_AXES, None)
    repl_spec = P()
    return jax.shard_map(functools.partial(device_step, num_dev), mesh=mesh, in_specs=(row_spec, row_spec, repl_spec, repl_spec, repl_spec, repl_spec, repl_spec, repl_spec, repl_spec, repl_spec), out_specs=(repl_spec, repl_spec, repl_spec, repl_spec, repl_spec, repl_spec, repl_spec, repl_spec), check_vma=False)
```

```python
import functools
import jax
import jax.numpy as jnp
from jax import lax
from jax.experimental import pallas as pl
from jax.experimental.pallas import tpu as pltpu
from jax.sharding import PartitionSpec as P

BN_EPS = 1e-5
ROW_AXES = ('pod', 'data')
MESH = pl.DeviceIdType.MESH
WIDTH = 2048
QCOLS = WIDTH // 4
CHUNK = 128
BLOCK = CHUNK // 2


def coordinates():
    pod, dat = lax.axis_index('pod'), lax.axis_index('data')
    return lax.div(pod, 2), lax.rem(pod, 2), lax.div(dat, 2), lax.rem(dat, 2)


def device(z, y, x, c):
    return (z * 2 + y, x * 2 + c)


def remote(src, dst, send, recv, dev):
    copy = pltpu.make_async_remote_copy(src_ref=src, dst_ref=dst, send_sem=send, recv_sem=recv, device_id=dev, device_id_type=MESH)
    copy.start()
    return copy


def meet(peers):
    barrier = pltpu.get_barrier_semaphore()
    for dev in peers:
        pl.semaphore_signal(barrier, inc=1, device_id=dev, device_id_type=MESH)
    pl.semaphore_wait(barrier, len(peers))


class StatSum:
    def __init__(self, half, v_ref, o_ref, from_core, plane, line, send, recv):
        z, y, x, c = coordinates()
        self.core_peer = device(z, y, x, 1 - c)
        self.plane_peers = [device(z, y, 1 - x, c), device(z, 1 - y, x, c), device(z, 1 - y, 1 - x, c)]
        self.line_peers = [device(lax.rem(z + o, 4), y, x, c) for o in (1, 2, 3)]
        self.mine = pl.ds(pl.multiple_of(c * half, 128), half)
        self.theirs = pl.ds(pl.multiple_of((1 - c) * half, 128), half)
        self.spot, self.z = y * 2 + x, z
        self.refs, self.sems, self.copies = (v_ref, o_ref, from_core, plane, line), (send, recv), []

    def peers(self):
        return [self.core_peer] + self.plane_peers + self.line_peers

    def send(self, src, dst, devs):
        for dev in devs:
            i = len(self.copies)
            self.copies.append(remote(src, dst, self.sems[0].at[i], self.sems[1].at[i], dev))

    def arrived(self, first, last):
        for copy in self.copies[first:last]:
            copy.wait_recv()

    def step(self, i):
        v_ref, o_ref, from_core, plane, line = self.refs
        if i == 0:
            self.send(v_ref.at[:, self.theirs], from_core, [self.core_peer])
        elif i == 1:
            self.arrived(0, 1)
            plane[self.spot] = v_ref[:, self.mine] + from_core[...]
            self.send(plane.at[self.spot], plane.at[self.spot], self.plane_peers)
        elif i == 2:
            self.arrived(1, 4)
            line[self.z] = (plane[0] + plane[1]) + (plane[2] + plane[3])
            self.send(line.at[self.z], line.at[self.z], self.line_peers)
        elif i == 3:
            self.arrived(4, 7)
            o_ref[:, self.mine] = (line[0] + line[1]) + (line[2] + line[3])
            self.send(o_ref.at[:, self.mine], o_ref.at[:, self.mine], [self.core_peer])
        else:
            self.arrived(7, 8)
            for copy in self.copies:
                copy.wait_send()


def stat_kernel(half, *refs):
    total = StatSum(half, *refs)
    meet(total.peers())
    for i in range(5):
        total.step(i)


def sum_stats(values, collective_id):
    rows, width = values.shape
    half = width // 2
    return pl.pallas_call(
        functools.partial(stat_kernel, half),
        out_shape=jax.ShapeDtypeStruct((rows, width), jnp.float32),
        in_specs=[pl.BlockSpec(memory_space=pltpu.VMEM)],
        out_specs=pl.BlockSpec(memory_space=pltpu.VMEM),
        scratch_shapes=[pltpu.VMEM((rows, half), jnp.float32), pltpu.VMEM((4, rows, half), jnp.float32), pltpu.VMEM((4, rows, half), jnp.float32),
                        pltpu.SemaphoreType.DMA((8,)), pltpu.SemaphoreType.DMA((8,))],
        compiler_params=pltpu.CompilerParams(collective_id=collective_id, has_side_effects=True),
    )(values)


TAPER = (32, 64, 96)
RING = 1024


def chunk_plan(row_counts, late):
    plan, base = [], 0
    for a, rows in enumerate(row_counts):
        left = rows // 2
        head = list(TAPER) if a == 0 else []
        tail = list(TAPER[::-1]) if a == len(row_counts) - 1 else []
        left -= sum(head) + sum(tail)
        row = 0
        for size in head + [CHUNK] * (left // CHUNK) + ([left % CHUNK] if left % CHUNK else []) + tail:
            plan.append((a, row, base % RING, size // 2, 1 if len(plan) % late == late - 1 else 0))
            row, base = row + size, base + size
    return plan


def reduce_kernel(row_counts, plan, num_rows, work, *refs):
    count = len(row_counts)
    make_grad = num_rows is not None
    if work:
        extra, refs = refs[:WORK_INPUTS], refs[WORK_INPUTS:]
    else:
        parts, refs = refs[:count], refs[count:]
    if make_grad:
        lam_ref, refs = refs[0], refs[1:]
    outs, refs = refs[:count], refs[count:]
    if work:
        parts, extra, refs = refs[:count], extra + refs[:WORK_OUTPUTS], refs[WORK_OUTPUTS:]
    if make_grad:
        loss_ref, refs = refs[0], refs[1:]
    own, from_core, recv_first, recv_second, recv_third, send, recv, core_send, core_recv, local_sem = refs[:10]
    if make_grad:
        shard = refs[10]
        loss_ref[...] = jnp.zeros_like(loss_ref)
    z, y, x, c = coordinates()
    core_peer = device(z, y, x, 1 - c)
    flat_peer = {'x': device(z, y, 1 - x, c), 'y': device(z, 1 - y, x, c)}
    flat_pos = {'x': x, 'y': y}
    line_peers = [device(lax.rem(z + o, 4), y, x, c) for o in (1, 2, 3)]
    plane_peers = [flat_peer['x'], flat_peer['y'], device(z, 1 - y, 1 - x, c)]
    meet([core_peer] + (plane_peers if work else plane_peers[:2]) + line_peers)
    hooks = work(extra + refs[10:]) if work else {}
    chunks = len(plan)
    sends = {}
    order = lambda kind, j: (('x', 'y', 'z'), ('y', 'x', 'z'))[j] if kind == 0 else (('x', 'z', 'y'), ('y', 'z', 'x'))[j]
    state = {}

    def start(k):
        a, row, base, size, _ = plan[k]
        sends[k] = []
        for old in list(sends):
            if old < k and plan[old][2] < base + 2 * size and base < plan[old][2] + 2 * plan[old][3]:
                finish(old)
        half = row_counts[a] // 2
        mine = pl.ds(pl.multiple_of(c * half + row, 16), 2 * size)
        theirs = pl.ds(pl.multiple_of((1 - c) * half + row, 16), 2 * size)
        load = pltpu.make_async_copy(parts[a].at[mine], own.at[pl.ds(base, 2 * size)], local_sem.at[k, 2])
        load.start()
        copy = remote(parts[a].at[theirs], from_core.at[pl.ds(base, 2 * size)], core_send.at[k, 0], core_recv.at[k, 0], core_peer)
        sends[k].append(copy)
        state[k] = {'load': load, 'core': copy}
        for j in range(2):
            state[k, j] = dict(rows=pl.ds(base + j * size, size), out=row + j * size, size=size, col=0, cols=WIDTH)

    def finish(k):
        state[k]['pair'].wait_recv()
        for copy in sends.pop(k):
            copy.wait_send()

    def columns(s):
        return pl.ds(s['col'] if isinstance(s['col'], int) else pl.multiple_of(s['col'], 128), s['cols'])

    def at(s):
        return s['rows'], columns(s)

    def scatter(k, j, step):
        dims = order(plan[k][4], j)
        dim = dims[step]
        s = state[k, j]
        base = 0 if step == 0 else (1 if step == 1 else 2 if dims[1] != 'z' else 4)
        buffer = (recv_first, recv_second, recv_third)[step]
        cols = s['cols'] // (4 if dim == 'z' else 2)
        copies, lands = [], []
        spots = [(lax.rem(z + o, 4), line_peers[o - 1]) for o in (1, 2, 3)] if dim == 'z' else [(1 - flat_pos[dim], flat_peer[dim])]
        for i, (spot, dev) in enumerate(spots):
            land = buffer.at[s['rows'], pl.ds(i * cols, cols)]
            part = dict(s, col=s['col'] + spot * cols, cols=cols)
            copies.append(remote(own.at[at(part)], land, send.at[k, j, base + i], recv.at[k, j, base + i], dev))
            lands.append(land)
        s.update(col=s['col'] + (z if dim == 'z' else flat_pos[dim]) * cols, cols=cols, copies=copies, lands=lands)
        sends[k].extend(copies)

    def absorb(k, j):
        s = state[k, j]
        for copy in s['copies']:
            copy.wait_recv()
        lands = [land[...] for land in s['lands']]
        total = own[at(s)] + lands[0]
        if len(lands) == 3:
            total = total + (lands[1] + lands[2])
        return total

    def first(k):
        _, _, base, size, _ = plan[k]
        state[k]['load'].wait()
        state[k]['core'].wait_recv()
        rows = pl.ds(base, 2 * size)
        own[rows] = own[rows] + from_core[rows]
        for j in range(2):
            scatter(k, j, 0)

    def middle(step, k):
        for j in range(2):
            own[at(state[k, j])] = absorb(k, j)
            scatter(k, j, step)

    def out_at(k, s):
        a = plan[k][0]
        row = c * (row_counts[a] // 2) + s['out']
        return outs[a].at[pl.ds(pl.multiple_of(row, 16), s['size']), columns(s)]

    def gather(k, j, step):
        dims = order(plan[k][4], j)
        dim = dims[2 - step]
        s = state[k, j]
        base = 5 + (0 if step == 0 else 4 if step == 2 else (1 if dims[2] != 'z' else 3))
        src = out_at(k, s) if step else s['src']
        dst = out_at(k, s)
        peers = line_peers if dim == 'z' else [flat_peer[dim]]
        copies = [remote(src, dst, send.at[k, j, base + i], recv.at[k, j, base + i], dev) for i, dev in enumerate(peers)]
        s.update(col=s['col'] - (z if dim == 'z' else flat_pos[dim]) * s['cols'], cols=(4 if dim == 'z' else 2) * s['cols'], copies=copies)
        if step == 2:
            s.update(col=0)
        sends[k].extend(copies)

    def turn(k):
        a = plan[k][0]
        for j in range(2):
            s = state[k, j]
            total = absorb(k, j)
            if make_grad:
                lam = lam_ref[0, 0]
                corr = total * (1.0 / num_rows)
                row = c * (row_counts[a] // 2) + s['out'] + lax.broadcasted_iota(jnp.int32, corr.shape, 0)
                col = s['col'] + lax.broadcasted_iota(jnp.int32, corr.shape, 1)
                diag = row == col
                miss = 1.0 - corr
                loss = jnp.where(diag, miss * miss, lam * (corr * corr))
                loss_ref[...] = loss_ref[...] + jnp.sum(loss.reshape(s['size'] // 8, 8, 128), axis=0)
                shard[s['rows']] = jnp.where(diag, -2.0 * miss, (2.0 * lam) * corr).astype(jnp.bfloat16)
                s['src'] = shard.at[s['rows']]
            else:
                own[at(s)] = total
                s['src'] = own.at[at(s)]
            s['keep'] = pltpu.make_async_copy(s['src'], out_at(k, s), local_sem.at[k, j])
            s['keep'].start()
            gather(k, j, 0)

    def spread(step, k):
        for j in range(2):
            s = state[k, j]
            for copy in s['copies']:
                copy.wait_recv()
            if step == 1:
                s['keep'].wait()
            gather(k, j, step)

    def pair(k):
        a, row, _, size, _ = plan[k]
        for j in range(2):
            for copy in state[k, j]['copies']:
                copy.wait_recv()
        rows = pl.ds(pl.multiple_of(c * (row_counts[a] // 2) + row, 16), 2 * size)
        copy = remote(outs[a].at[rows], outs[a].at[rows], core_send.at[k, 1], core_recv.at[k, 1], core_peer)
        sends[k].append(copy)
        state[k]['pair'] = copy

    stages = [first, functools.partial(middle, 1), functools.partial(middle, 2), turn, functools.partial(spread, 1), functools.partial(spread, 2), pair]
    for t in range(chunks + len(stages) - 1):
        for task in hooks.get(t, ()):
            task()
        for k in range(chunks):
            if t == (max(k - 1, 0) if work and k >= len(TAPER) else 0):
                start(k)
        for i, stage in enumerate(stages):
            if 0 <= t - i < chunks:
                stage(t - i)
    for k in list(sends):
        finish(k)


def reduce_all(parts, collective_id, lam=None, num_rows=None, late=3):
    row_counts = [p.shape[0] for p in parts]
    plan = chunk_plan(row_counts, late)
    chunks, rows = len(plan), sum(row_counts) // 2
    any_spec = pl.BlockSpec(memory_space=pl.ANY)
    make_grad = lam is not None
    out_type = jnp.bfloat16 if make_grad else jnp.float32
    in_specs = [any_spec] * len(parts)
    out_specs = [any_spec] * len(parts)
    out_shape = [jax.ShapeDtypeStruct(p.shape, out_type) for p in parts]
    args = list(parts)
    if make_grad:
        in_specs.append(pl.BlockSpec(memory_space=pltpu.SMEM))
        args.append(lam.reshape(1, 1))
        out_specs.append(pl.BlockSpec(memory_space=pltpu.VMEM))
        out_shape.append(jax.ShapeDtypeStruct((8, 128), jnp.float32))
    f32 = jnp.float32
    scratch = [
        pltpu.VMEM((rows, WIDTH), f32), pltpu.VMEM((rows, WIDTH), f32), pltpu.VMEM((rows, WIDTH // 2), f32),
        pltpu.VMEM((rows, 3 * WIDTH // 8), f32), pltpu.VMEM((rows, 3 * WIDTH // 16), f32),
        pltpu.SemaphoreType.DMA((chunks, 2, 10)), pltpu.SemaphoreType.DMA((chunks, 2, 10)),
        pltpu.SemaphoreType.DMA((chunks, 2)), pltpu.SemaphoreType.DMA((chunks, 2)), pltpu.SemaphoreType.DMA((chunks, 3)),
    ]
    if make_grad:
        scratch.append(pltpu.VMEM((rows, WIDTH // 16), jnp.bfloat16))
    return pl.pallas_call(
        functools.partial(reduce_kernel, row_counts, plan, num_rows if make_grad else None, None),
        out_shape=out_shape, in_specs=in_specs, out_specs=out_specs, scratch_shapes=scratch,
        compiler_params=pltpu.CompilerParams(collective_id=collective_id, has_side_effects=True, vmem_limit_bytes=56 * 1024 * 1024),
    )(*args)


WORK_INPUTS, WORK_OUTPUTS = 9, 5
TILE = 256
VIEW_ROWS = 512


def backward_work(num_rows, refs):
    grad_proj, hid_two, w_third, w_second, pre_two, pre_one, hid_one, feats, vec = refs[:9]
    part_third, part_second, part_first, total_two, total_one = refs[9:14]
    grad, act, w_buf, n_buf, x_buf, o_buf = refs[14:20]
    stat_two, stat_one = refs[20:26], refs[26:32]
    grad_sem, w_sem, n_sem, x_sem, o_sem = refs[32:37]
    rows_of = [pl.ds(v * VIEW_ROWS, VIEW_ROWS) for v in range(2)]
    sums = [StatSum(WIDTH // 2, st[0], tot, *st[1:]) for st, tot in ((stat_two, total_two), (stat_one, total_one))]

    def tile(i):
        return pl.ds(pl.multiple_of(i * TILE, TILE), TILE)

    def loop(first, last, fetch, body):
        for copy in fetch(first, first % 2):
            copy.start()

        def trip(i, carry):
            slot = lax.rem(i, 2)

            @pl.when(i + 1 < last)
            def _():
                for copy in fetch(i + 1, 1 - slot):
                    copy.start()
            for copy in fetch(i, slot):
                copy.wait()
            body(i, slot)
            return carry
        lax.fori_loop(first, last, trip, 0)

    def pre_copy(pre, i, slot):
        return pltpu.make_async_copy(pre.at[:, tile(i)], n_buf.at[slot], n_sem.at[slot])

    def normed(slot, v, first, cols):
        return (n_buf[slot, rows_of[v]] - vec[pl.ds(first + 4 + v, 1), cols]) * vec[pl.ds(first + 2 + v, 1), cols]

    def input_grad(layer, first, last):
        weight, pre = ((w_second, pre_one), (w_third, pre_two))[layer]
        stat = (stat_one, stat_two)[layer][0]
        g = 6 if layer == 0 else 0

        def fetch(i, slot):
            return [pltpu.make_async_copy(weight.at[tile(i)], w_buf.at[slot], w_sem.at[slot]), pre_copy(pre, i, slot)]

        def body(i, slot):
            cols = tile(i)
            for v in range(2):
                dx = lax.dot_general(grad[rows_of[v]], w_buf[slot], (((1,), (1,)), ((), ())), preferred_element_type=jnp.float32)
                n = normed(slot, v, g, cols)
                da = jnp.where(vec[pl.ds(g, 1), cols] * n + vec[pl.ds(g + 1, 1), cols] > 0, dx, 0.0)
                act[rows_of[v], cols] = da
                stat[pl.ds(v, 1), cols] = jnp.sum(da * n, axis=0, keepdims=True)
                stat[pl.ds(2 + v, 1), cols] = jnp.sum(da, axis=0, keepdims=True)
        loop(first, last, fetch, body)

    def norm_grad(layer):
        pre, total = ((pre_one, total_one), (pre_two, total_two))[layer]
        g = 6 if layer == 0 else 0

        def body(i, slot):
            cols = tile(i)
            for v in range(2):
                cross = total[pl.ds(v, 1), cols] * (1.0 / num_rows)
                mean = total[pl.ds(2 + v, 1), cols] * (1.0 / num_rows)
                scale = vec[pl.ds(g, 1), cols] * vec[pl.ds(g + 2 + v, 1), cols]
                grad[rows_of[v], cols] = (scale * (act[rows_of[v], cols] - mean - normed(slot, v, g, cols) * cross)).astype(jnp.bfloat16)
        loop(0, WIDTH // TILE, lambda i, slot: [pre_copy(pre, i, slot)], body)

    def weight_grad(hidden, out, first, last):
        tiles = out.shape[0] // TILE
        spot = lambda i: lax.div(i, 2) + lax.rem(i, 2) * (tiles // 2)

        def fetch(i, slot):
            return [pltpu.make_async_copy(hidden.at[:, tile(spot(i))], x_buf.at[slot], x_sem.at[slot])]

        def put(i, slot):
            return pltpu.make_async_copy(o_buf.at[slot], out.at[tile(spot(i))], o_sem.at[slot])

        def body(i, slot):
            @pl.when(i >= first + 2)
            def _():
                put(i, slot).wait()
            for n in range(4):
                cols = pl.ds(n * (WIDTH // 4), WIDTH // 4)
                o_buf[slot, :, cols] = lax.dot_general(x_buf[slot], grad[:, cols], (((0,), (0,)), ((), ())), preferred_element_type=jnp.float32)
            put(i, slot).start()
        loop(first, last, fetch, body)
        for i in (last - 2, last - 1):
            put(i, i % 2).wait()

    grad_load = pltpu.make_async_copy(grad_proj, grad, grad_sem)
    grad_load.start()
    step = lambda which, i: functools.partial(sums[which].step, i)
    run = functools.partial
    return {
        0: [grad_load.wait, run(weight_grad, hid_two, part_third, 0, 2)], 1: [run(weight_grad, hid_two, part_third, 2, 4)],
        2: [run(weight_grad, hid_two, part_third, 4, 8)], 3: [run(input_grad, 1, 0, 4)], 4: [run(input_grad, 1, 4, 8), step(0, 0)],
        5: [step(0, 1)], 6: [step(0, 2)], 7: [step(0, 3)], 8: [step(0, 4), run(norm_grad, 1)],
        9: [run(weight_grad, hid_one, part_second, 0, 4)], 10: [run(weight_grad, hid_one, part_second, 4, 8)],
        11: [run(input_grad, 0, 0, 4)], 12: [run(input_grad, 0, 4, 8), step(1, 0)],
        13: [step(1, 1)], 14: [step(1, 2)], 15: [step(1, 3)], 16: [step(1, 4), run(norm_grad, 0)], 17: [run(weight_grad, feats, part_first, 0, 2)],
    }


def reduce_with_backward(work_inputs, collective_id, num_rows):
    row_counts = [WIDTH, WIDTH, WIDTH // 4]
    plan = chunk_plan(row_counts, 3)
    chunks, rows, views = len(plan), RING, 2 * VIEW_ROWS
    any_spec, vmem_spec = pl.BlockSpec(memory_space=pl.ANY), pl.BlockSpec(memory_space=pltpu.VMEM)
    f32, bf16, dma = jnp.float32, jnp.bfloat16, pltpu.SemaphoreType.DMA
    half = WIDTH // 2
    stat = [pltpu.VMEM((4, WIDTH), f32), pltpu.VMEM((4, half), f32), pltpu.VMEM((4, 4, half), f32), pltpu.VMEM((4, 4, half), f32), dma((8,)), dma((8,))]
    scratch = [
        pltpu.VMEM((rows, WIDTH), f32), pltpu.VMEM((rows, WIDTH), f32), pltpu.VMEM((rows, WIDTH // 2), f32),
        pltpu.VMEM((rows, 3 * WIDTH // 8), f32), pltpu.VMEM((rows, 3 * WIDTH // 16), f32),
        dma((chunks, 2, 10)), dma((chunks, 2, 10)), dma((chunks, 2)), dma((chunks, 2)), dma((chunks, 3)),
        pltpu.VMEM((views, WIDTH), bf16), pltpu.VMEM((views, WIDTH), f32), pltpu.VMEM((2, TILE, WIDTH), bf16), pltpu.VMEM((2, views, TILE), f32),
        pltpu.VMEM((2, views, TILE), bf16), pltpu.VMEM((2, TILE, WIDTH), f32),
        *stat, *stat, dma, dma((2,)), dma((2,)), dma((2,)), dma((2,)),
    ]
    shape = jax.ShapeDtypeStruct
    return pl.pallas_call(
        functools.partial(reduce_kernel, row_counts, plan, None, functools.partial(backward_work, num_rows)),
        out_shape=[shape((r, WIDTH), f32) for r in row_counts + row_counts] + [shape((4, WIDTH), f32)] * 2,
        in_specs=[any_spec] * 8 + [vmem_spec], out_specs=[any_spec] * 6 + [vmem_spec] * 2, scratch_shapes=scratch,
        compiler_params=pltpu.CompilerParams(collective_id=collective_id, has_side_effects=True, vmem_limit_bytes=62 * 1024 * 1024),
    )(*work_inputs)


def total_stats(first, second, collective_id):
    local = jnp.concatenate([first, second])
    return sum_stats(local, collective_id).reshape(2, 2, WIDTH)


def batch_norm(pre_act, num_rows):
    totals = total_stats(jnp.sum(pre_act, axis=1), jnp.sum(pre_act * pre_act, axis=1), 0) / num_rows
    inv_std = lax.rsqrt(totals[1] - totals[0] * totals[0] + BN_EPS)
    return (pre_act - totals[0][:, None, :]) * inv_std[:, None, :], totals[0], inv_std


def run_layer(hidden, weight, gain_vec, shift_vec, num_rows):
    pre_act = jnp.einsum('vnf,fd->vnd', hidden, weight, preferred_element_type=jnp.float32)
    normed, mean, inv_std = batch_norm(pre_act, num_rows)
    post_affine = gain_vec * normed + shift_vec
    return jnp.maximum(post_affine, 0.0).astype(jnp.bfloat16), pre_act, jnp.concatenate([gain_vec[None], shift_vec[None], inv_std, mean])


def device_step(num_dev, feat_a, feat_b, w_first, w_second, w_third, gain_first, shift_first, gain_second, shift_second, lam_off):
    num_rows = feat_a.shape[0] * num_dev
    both_views = jnp.stack([feat_a, feat_b])
    hid_one, pre_one, vec_one = run_layer(both_views, w_first, gain_first, shift_first, num_rows)
    hid_two, pre_two, vec_two = run_layer(hid_one, w_second, gain_second, shift_second, num_rows)
    proj_out = jnp.einsum('vnf,fd->vnd', hid_two, w_third, preferred_element_type=jnp.float32)
    emb_norm, _, inv_three = batch_norm(proj_out, num_rows)
    inv_three = inv_three[:, None, :]
    emb_bf = emb_norm.astype(jnp.bfloat16)
    corr_part = lax.dot_general(emb_bf[0], emb_bf[1], (((0,), (0,)), ((), ())), preferred_element_type=jnp.float32)
    grad_corr, loss_part = reduce_all([corr_part], 2, lam_off, num_rows)
    grad_emb_a = lax.dot_general(emb_bf[1], grad_corr, (((1,), (1,)), ((), ())), preferred_element_type=jnp.float32)
    grad_emb_b = jnp.dot(emb_bf[0], grad_corr, preferred_element_type=jnp.float32)
    grad_emb = jnp.stack([grad_emb_a, grad_emb_b]) / num_rows
    local = jnp.concatenate([jnp.sum(grad_emb, axis=1), jnp.sum(grad_emb * emb_norm, axis=1)])
    extra = jnp.full((4, 256), jnp.sum(loss_part), jnp.float32)
    totals = sum_stats(jnp.concatenate([local, extra], axis=1), 1)
    total_loss = totals[0, WIDTH]
    totals = totals[:, :WIDTH].reshape(2, 2, WIDTH) / num_rows
    grad_proj = (inv_three * (grad_emb - totals[0][:, None, :] - emb_norm * totals[1][:, None, :])).astype(jnp.bfloat16)
    flat = lambda t: t.reshape(-1, t.shape[-1])
    grad_third, grad_second, grad_first, _, _, _, total_two, total_one = reduce_with_backward(
        [flat(grad_proj), flat(hid_two), w_third, w_second, flat(pre_two), flat(pre_one), flat(hid_one), flat(both_views), jnp.concatenate([vec_two, vec_one])],
        3, num_rows)
    grad_gain_second, grad_shift_second = total_two[0] + total_two[1], total_two[2] + total_two[3]
    grad_gain_first, grad_shift_first = total_one[0] + total_one[1], total_one[2] + total_one[3]
    return (total_loss, grad_first, grad_second, grad_third, grad_gain_first, grad_shift_first, grad_gain_second, grad_shift_second)


def solution(mesh):
    num_dev = mesh.shape['pod'] * mesh.shape['data']
    row_spec = P(ROW_AXES, None)
    repl_spec = P()
    return jax.shard_map(functools.partial(device_step, num_dev), mesh=mesh, in_specs=(row_spec, row_spec, repl_spec, repl_spec, repl_spec, repl_spec, repl_spec, repl_spec, repl_spec, repl_spec), out_specs=(repl_spec, repl_spec, repl_spec, repl_spec, repl_spec, repl_spec, repl_spec, repl_spec), check_vma=False)
```

```python
import functools
import jax
import jax.numpy as jnp
from jax import lax
from jax.experimental import pallas as pl
from jax.experimental.pallas import tpu as pltpu
from jax.sharding import PartitionSpec as P

BN_EPS = 1e-5
ROW_AXES = ('pod', 'data')
MESH = pl.DeviceIdType.MESH
WIDTH = 2048
QCOLS = WIDTH // 4
CHUNK = 128
BLOCK = CHUNK // 2


def coordinates():
    pod, dat = lax.axis_index('pod'), lax.axis_index('data')
    return lax.div(pod, 2), lax.rem(pod, 2), lax.div(dat, 2), lax.rem(dat, 2)


def device(z, y, x, c):
    return (z * 2 + y, x * 2 + c)


def remote(src, dst, send, recv, dev):
    copy = pltpu.make_async_remote_copy(src_ref=src, dst_ref=dst, send_sem=send, recv_sem=recv, device_id=dev, device_id_type=MESH)
    copy.start()
    return copy


def meet(peers):
    barrier = pltpu.get_barrier_semaphore()
    for dev in peers:
        pl.semaphore_signal(barrier, inc=1, device_id=dev, device_id_type=MESH)
    pl.semaphore_wait(barrier, len(peers))


class StatSum:
    def __init__(self, half, v_ref, o_ref, from_core, plane, line, send, recv):
        z, y, x, c = coordinates()
        self.core_peer = device(z, y, x, 1 - c)
        self.plane_peers = [device(z, y, 1 - x, c), device(z, 1 - y, x, c), device(z, 1 - y, 1 - x, c)]
        self.line_peers = [device(lax.rem(z + o, 4), y, x, c) for o in (1, 2, 3)]
        self.mine = pl.ds(pl.multiple_of(c * half, 128), half)
        self.theirs = pl.ds(pl.multiple_of((1 - c) * half, 128), half)
        self.spot, self.z = y * 2 + x, z
        self.refs, self.sems, self.copies = (v_ref, o_ref, from_core, plane, line), (send, recv), []

    def peers(self):
        return [self.core_peer] + self.plane_peers + self.line_peers

    def send(self, src, dst, devs):
        for dev in devs:
            i = len(self.copies)
            self.copies.append(remote(src, dst, self.sems[0].at[i], self.sems[1].at[i], dev))

    def arrived(self, first, last):
        for copy in self.copies[first:last]:
            copy.wait_recv()

    def step(self, i):
        v_ref, o_ref, from_core, plane, line = self.refs
        if i == 0:
            self.send(v_ref.at[:, self.theirs], from_core, [self.core_peer])
        elif i == 1:
            self.arrived(0, 1)
            plane[self.spot] = v_ref[:, self.mine] + from_core[...]
            self.send(plane.at[self.spot], plane.at[self.spot], self.plane_peers)
        elif i == 2:
            self.arrived(1, 4)
            line[self.z] = (plane[0] + plane[1]) + (plane[2] + plane[3])
            self.send(line.at[self.z], line.at[self.z], self.line_peers)
        elif i == 3:
            self.arrived(4, 7)
            o_ref[:, self.mine] = (line[0] + line[1]) + (line[2] + line[3])
            self.send(o_ref.at[:, self.mine], o_ref.at[:, self.mine], [self.core_peer])
        else:
            self.arrived(7, 8)
            for copy in self.copies:
                copy.wait_send()


def stat_kernel(half, *refs):
    total = StatSum(half, *refs)
    meet(total.peers())
    for i in range(5):
        total.step(i)


def sum_stats(values, collective_id):
    rows, width = values.shape
    half = width // 2
    return pl.pallas_call(
        functools.partial(stat_kernel, half),
        out_shape=jax.ShapeDtypeStruct((rows, width), jnp.float32),
        in_specs=[pl.BlockSpec(memory_space=pltpu.VMEM)],
        out_specs=pl.BlockSpec(memory_space=pltpu.VMEM),
        scratch_shapes=[pltpu.VMEM((rows, half), jnp.float32), pltpu.VMEM((4, rows, half), jnp.float32), pltpu.VMEM((4, rows, half), jnp.float32),
                        pltpu.SemaphoreType.DMA((8,)), pltpu.SemaphoreType.DMA((8,))],
        compiler_params=pltpu.CompilerParams(collective_id=collective_id, has_side_effects=True),
    )(values)


TAPER = (32, 64, 96)
RING = 1024
ORDERS = (('x', 'y', 'z'), ('y', 'x', 'z'), ('x', 'z', 'y'), ('y', 'z', 'x'))
SHARES = {4: {128: (40, 40, 24, 24)}, 2: {128: (48, 48, 16, 16), 96: (32, 32, 16, 16), 64: (32, 32, 0, 0), 32: (16, 16, 0, 0)}}
MIXED = (1,)


def chunk_plan(row_counts, itemsize):
    plan, base = [], 0
    for a, rows in enumerate(row_counts):
        left = rows // 2
        head = list(TAPER) if a == 0 else []
        tail = list(TAPER[::-1]) if a == len(row_counts) - 1 else []
        left -= sum(head) + sum(tail)
        row = 0
        for size in head + [CHUNK] * (left // CHUNK) + ([left % CHUNK] if left % CHUNK else []) + tail:
            two = (size // 2, size // 2, 0, 0)
            mixed = len(row_counts) == 1 or a in MIXED
            plan.append((a, row, base % RING, size, SHARES[itemsize].get(size, two) if mixed else two))
            row, base = row + size, base + size
    return plan


def reduce_kernel(row_counts, plan, num_rows, work, *refs):
    count = len(row_counts)
    make_grad = num_rows is not None
    if work:
        extra, refs = refs[:WORK_INPUTS], refs[WORK_INPUTS:]
    else:
        parts, refs = refs[:count], refs[count:]
    if make_grad:
        lam_ref, refs = refs[0], refs[1:]
    outs, refs = refs[:count], refs[count:]
    if work:
        parts, extra, refs = refs[:count], extra + refs[:WORK_OUTPUTS], refs[WORK_OUTPUTS:]
    if make_grad:
        loss_ref, refs = refs[0], refs[1:]
    own, from_core, recv_first, recv_second, recv_third, send, recv, core_send, core_recv, local_sem = refs[:10]
    if make_grad:
        shard = refs[10]
        loss_ref[...] = jnp.zeros_like(loss_ref)
    z, y, x, c = coordinates()
    core_peer = device(z, y, x, 1 - c)
    flat_peer = {'x': device(z, y, 1 - x, c), 'y': device(z, 1 - y, x, c)}
    flat_pos = {'x': x, 'y': y}
    line_peers = [device(lax.rem(z + o, 4), y, x, c) for o in (1, 2, 3)]
    plane_peers = [flat_peer['x'], flat_peer['y'], device(z, 1 - y, 1 - x, c)]
    meet([core_peer] + (plane_peers if work else plane_peers[:2]) + line_peers)
    hooks = work(extra + refs[10:]) if work else {}
    chunks = len(plan)
    sends = {}
    parts_of = lambda k: [j for j in range(4) if plan[k][4][j]]
    align = 16 if make_grad else 8
    state = {}

    def start(k):
        a, row, base, size, shares = plan[k]
        sends[k] = []
        for old in list(sends):
            if old < k and plan[old][2] < base + size and base < plan[old][2] + plan[old][3]:
                finish(old)
        half = row_counts[a] // 2
        mine = pl.ds(pl.multiple_of(c * half + row, 16), size)
        theirs = pl.ds(pl.multiple_of((1 - c) * half + row, 16), size)
        load = pltpu.make_async_copy(parts[a].at[mine], own.at[pl.ds(base, size)], local_sem.at[k, 4])
        load.start()
        copy = remote(parts[a].at[theirs], from_core.at[pl.ds(base, size)], core_send.at[k, 0], core_recv.at[k, 0], core_peer)
        sends[k].append(copy)
        state[k] = {'load': load, 'core': copy}
        for j in parts_of(k):
            skip = sum(shares[:j])
            state[k, j] = dict(rows=pl.ds(base + skip, shares[j]), out=row + skip, size=shares[j], col=0, cols=WIDTH)

    def finish(k):
        state[k]['pair'].wait_recv()
        for copy in sends.pop(k):
            copy.wait_send()

    def columns(s):
        return pl.ds(s['col'] if isinstance(s['col'], int) else pl.multiple_of(s['col'], 128), s['cols'])

    def at(s):
        return s['rows'], columns(s)

    def scatter(k, j, step):
        dims = ORDERS[j]
        dim = dims[step]
        s = state[k, j]
        base = 0 if step == 0 else (1 if step == 1 else 2 if dims[1] != 'z' else 4)
        buffer = (recv_first, recv_second, recv_third)[step]
        cols = s['cols'] // (4 if dim == 'z' else 2)
        copies, lands = [], []
        spots = [(lax.rem(z + o, 4), line_peers[o - 1]) for o in (1, 2, 3)] if dim == 'z' else [(1 - flat_pos[dim], flat_peer[dim])]
        for i, (spot, dev) in enumerate(spots):
            land = buffer.at[s['rows'], pl.ds(i * cols, cols)]
            part = dict(s, col=s['col'] + spot * cols, cols=cols)
            copies.append(remote(own.at[at(part)], land, send.at[k, j, base + i], recv.at[k, j, base + i], dev))
            lands.append(land)
        s.update(col=s['col'] + (z if dim == 'z' else flat_pos[dim]) * cols, cols=cols, copies=copies, lands=lands)
        sends[k].extend(copies)

    def absorb(k, j):
        s = state[k, j]
        for copy in s['copies']:
            copy.wait_recv()
        lands = [land[...] for land in s['lands']]
        total = own[at(s)] + lands[0]
        if len(lands) == 3:
            total = total + (lands[1] + lands[2])
        return total

    def first(k):
        _, _, base, size, _ = plan[k]
        state[k]['load'].wait()
        state[k]['core'].wait_recv()
        rows = pl.ds(base, size)
        own[rows] = own[rows] + from_core[rows]
        for j in parts_of(k):
            scatter(k, j, 0)

    def middle(step, k):
        for j in parts_of(k):
            own[at(state[k, j])] = absorb(k, j)
            scatter(k, j, step)

    def out_at(k, s):
        a = plan[k][0]
        row = c * (row_counts[a] // 2) + s['out']
        return outs[a].at[pl.ds(pl.multiple_of(row, align), s['size']), columns(s)]

    def gather(k, j, step):
        dims = ORDERS[j]
        dim = dims[2 - step]
        s = state[k, j]
        base = 5 + (0 if step == 0 else 4 if step == 2 else (1 if dims[2] != 'z' else 3))
        src = out_at(k, s) if step else s['src']
        dst = out_at(k, s)
        peers = line_peers if dim == 'z' else [flat_peer[dim]]
        copies = [remote(src, dst, send.at[k, j, base + i], recv.at[k, j, base + i], dev) for i, dev in enumerate(peers)]
        s.update(col=s['col'] - (z if dim == 'z' else flat_pos[dim]) * s['cols'], cols=(4 if dim == 'z' else 2) * s['cols'], copies=copies)
        if step == 2:
            s.update(col=0)
        sends[k].extend(copies)

    def turn(k):
        a = plan[k][0]
        for j in parts_of(k):
            s = state[k, j]
            total = absorb(k, j)
            if make_grad:
                lam = lam_ref[0, 0]
                corr = total * (1.0 / num_rows)
                row = c * (row_counts[a] // 2) + s['out'] + lax.broadcasted_iota(jnp.int32, corr.shape, 0)
                col = s['col'] + lax.broadcasted_iota(jnp.int32, corr.shape, 1)
                diag = row == col
                miss = 1.0 - corr
                loss = jnp.where(diag, miss * miss, lam * (corr * corr))
                loss_ref[...] = loss_ref[...] + jnp.sum(loss.reshape(s['size'] // 8, 8, 128), axis=0)
                shard[s['rows']] = jnp.where(diag, -2.0 * miss, (2.0 * lam) * corr).astype(jnp.bfloat16)
                s['src'] = shard.at[s['rows']]
            else:
                own[at(s)] = total
                s['src'] = own.at[at(s)]
            s['keep'] = pltpu.make_async_copy(s['src'], out_at(k, s), local_sem.at[k, j])
            s['keep'].start()
            gather(k, j, 0)

    def spread(step, k):
        for j in parts_of(k):
            s = state[k, j]
            for copy in s['copies']:
                copy.wait_recv()
            if step == 1:
                s['keep'].wait()
            gather(k, j, step)

    def pair(k):
        a, row, _, size, _ = plan[k]
        for j in parts_of(k):
            for copy in state[k, j]['copies']:
                copy.wait_recv()
        rows = pl.ds(pl.multiple_of(c * (row_counts[a] // 2) + row, 16), size)
        copy = remote(outs[a].at[rows], outs[a].at[rows], core_send.at[k, 1], core_recv.at[k, 1], core_peer)
        sends[k].append(copy)
        state[k]['pair'] = copy

    stages = [first, functools.partial(middle, 1), functools.partial(middle, 2), turn, functools.partial(spread, 1), functools.partial(spread, 2), pair]
    for t in range(chunks + len(stages) - 1):
        for task in hooks.get(t, ()) if t == 0 else ():
            task()
        for k in range(chunks):
            if t == (max(k - 1, 0) if work and k >= len(TAPER) else 0):
                start(k)
        for i, stage in enumerate(stages):
            if 0 <= t - i < chunks:
                stage(t - i)
            if i == 2 and t:
                for task in hooks.get(t, ()):
                    task()
    for k in list(sends):
        finish(k)


def reduce_all(parts, collective_id, lam=None, num_rows=None):
    row_counts = [p.shape[0] for p in parts]
    plan = chunk_plan(row_counts, 2 if lam is not None else 4)
    chunks, rows = len(plan), sum(row_counts) // 2
    any_spec = pl.BlockSpec(memory_space=pl.ANY)
    make_grad = lam is not None
    out_type = jnp.bfloat16 if make_grad else jnp.float32
    in_specs = [any_spec] * len(parts)
    out_specs = [any_spec] * len(parts)
    out_shape = [jax.ShapeDtypeStruct(p.shape, out_type) for p in parts]
    args = list(parts)
    if make_grad:
        in_specs.append(pl.BlockSpec(memory_space=pltpu.SMEM))
        args.append(lam.reshape(1, 1))
        out_specs.append(pl.BlockSpec(memory_space=pltpu.VMEM))
        out_shape.append(jax.ShapeDtypeStruct((8, 128), jnp.float32))
    f32 = jnp.float32
    scratch = [
        pltpu.VMEM((rows, WIDTH), f32), pltpu.VMEM((rows, WIDTH), f32), pltpu.VMEM((rows, WIDTH // 2), f32),
        pltpu.VMEM((rows, 3 * WIDTH // 8), f32), pltpu.VMEM((rows, 3 * WIDTH // 16), f32),
        pltpu.SemaphoreType.DMA((chunks, 4, 10)), pltpu.SemaphoreType.DMA((chunks, 4, 10)),
        pltpu.SemaphoreType.DMA((chunks, 2)), pltpu.SemaphoreType.DMA((chunks, 2)), pltpu.SemaphoreType.DMA((chunks, 5)),
    ]
    if make_grad:
        scratch.append(pltpu.VMEM((rows, WIDTH // 16), jnp.bfloat16))
    return pl.pallas_call(
        functools.partial(reduce_kernel, row_counts, plan, num_rows if make_grad else None, None),
        out_shape=out_shape, in_specs=in_specs, out_specs=out_specs, scratch_shapes=scratch,
        compiler_params=pltpu.CompilerParams(collective_id=collective_id, has_side_effects=True, vmem_limit_bytes=56 * 1024 * 1024),
    )(*args)


WORK_INPUTS, WORK_OUTPUTS = 9, 5
TILE = 256
VIEW_ROWS = 512


def backward_work(num_rows, refs):
    grad_proj, hid_two, w_third, w_second, pre_two, pre_one, hid_one, feats, vec = refs[:9]
    part_third, part_second, part_first, total_two, total_one = refs[9:14]
    grad, act, w_buf, n_buf, x_buf, o_buf = refs[14:20]
    stat_two, stat_one = refs[20:26], refs[26:32]
    grad_sem, w_sem, n_sem, x_sem, o_sem = refs[32:37]
    rows_of = [pl.ds(v * VIEW_ROWS, VIEW_ROWS) for v in range(2)]
    sums = [StatSum(WIDTH // 2, st[0], tot, *st[1:]) for st, tot in ((stat_two, total_two), (stat_one, total_one))]

    def tile(i):
        return pl.ds(pl.multiple_of(i * TILE, TILE), TILE)

    def loop(first, last, fetch, body):
        for copy in fetch(first, first % 2):
            copy.start()

        def trip(i, carry):
            slot = lax.rem(i, 2)

            @pl.when(i + 1 < last)
            def _():
                for copy in fetch(i + 1, 1 - slot):
                    copy.start()
            for copy in fetch(i, slot):
                copy.wait()
            body(i, slot)
            return carry
        lax.fori_loop(first, last, trip, 0)

    def pre_copy(pre, i, slot):
        return pltpu.make_async_copy(pre.at[:, tile(i)], n_buf.at[slot], n_sem.at[slot])

    def normed(slot, v, first, cols):
        return (n_buf[slot, rows_of[v]] - vec[pl.ds(first + 4 + v, 1), cols]) * vec[pl.ds(first + 2 + v, 1), cols]

    def input_grad(layer, first, last):
        weight, pre = ((w_second, pre_one), (w_third, pre_two))[layer]
        stat = (stat_one, stat_two)[layer][0]
        g = 6 if layer == 0 else 0

        def fetch(i, slot):
            return [pltpu.make_async_copy(weight.at[tile(i)], w_buf.at[slot], w_sem.at[slot]), pre_copy(pre, i, slot)]

        def body(i, slot):
            cols = tile(i)
            for v in range(2):
                dx = lax.dot_general(grad[rows_of[v]], w_buf[slot], (((1,), (1,)), ((), ())), preferred_element_type=jnp.float32)
                n = normed(slot, v, g, cols)
                da = jnp.where(vec[pl.ds(g, 1), cols] * n + vec[pl.ds(g + 1, 1), cols] > 0, dx, 0.0)
                act[rows_of[v], cols] = da
                stat[pl.ds(v, 1), cols] = jnp.sum(da * n, axis=0, keepdims=True)
                stat[pl.ds(2 + v, 1), cols] = jnp.sum(da, axis=0, keepdims=True)
        loop(first, last, fetch, body)

    def norm_grad(layer):
        pre, total = ((pre_one, total_one), (pre_two, total_two))[layer]
        g = 6 if layer == 0 else 0

        def body(i, slot):
            cols = tile(i)
            for v in range(2):
                cross = total[pl.ds(v, 1), cols] * (1.0 / num_rows)
                mean = total[pl.ds(2 + v, 1), cols] * (1.0 / num_rows)
                scale = vec[pl.ds(g, 1), cols] * vec[pl.ds(g + 2 + v, 1), cols]
                grad[rows_of[v], cols] = (scale * (act[rows_of[v], cols] - mean - normed(slot, v, g, cols) * cross)).astype(jnp.bfloat16)
        loop(0, WIDTH // TILE, lambda i, slot: [pre_copy(pre, i, slot)], body)

    def weight_grad(hidden, out, first, last):
        tiles = out.shape[0] // TILE
        spot = lambda i: lax.div(i, 2) + lax.rem(i, 2) * (tiles // 2)

        def fetch(i, slot):
            return [pltpu.make_async_copy(hidden.at[:, tile(spot(i))], x_buf.at[slot], x_sem.at[slot])]

        def put(i, slot):
            return pltpu.make_async_copy(o_buf.at[slot], out.at[tile(spot(i))], o_sem.at[slot])

        def body(i, slot):
            @pl.when(i >= first + 2)
            def _():
                put(i, slot).wait()
            for n in range(4):
                cols = pl.ds(n * (WIDTH // 4), WIDTH // 4)
                o_buf[slot, :, cols] = lax.dot_general(x_buf[slot], grad[:, cols], (((0,), (0,)), ((), ())), preferred_element_type=jnp.float32)
            put(i, slot).start()
        loop(first, last, fetch, body)
        for i in (last - 2, last - 1):
            put(i, i % 2).wait()

    grad_load = pltpu.make_async_copy(grad_proj, grad, grad_sem)
    grad_load.start()
    step = lambda which, i: functools.partial(sums[which].step, i)
    run = functools.partial
    return {
        0: [grad_load.wait, run(weight_grad, hid_two, part_third, 0, 2)], 1: [run(weight_grad, hid_two, part_third, 2, 4)],
        2: [run(weight_grad, hid_two, part_third, 4, 8)], 3: [run(input_grad, 1, 0, 4)], 4: [run(input_grad, 1, 4, 8), step(0, 0)],
        5: [step(0, 1)], 6: [step(0, 2)], 7: [step(0, 3)], 8: [step(0, 4), run(norm_grad, 1), run(weight_grad, hid_one, part_second, 0, 2)],
        9: [run(weight_grad, hid_one, part_second, 2, 8)],
        10: [run(input_grad, 0, 0, 4)], 11: [run(input_grad, 0, 4, 8), step(1, 0)],
        12: [step(1, 1)], 13: [step(1, 2)], 14: [step(1, 3)], 15: [step(1, 4), run(norm_grad, 0)], 16: [run(weight_grad, feats, part_first, 0, 2)],
    }


def reduce_with_backward(work_inputs, collective_id, num_rows):
    row_counts = [WIDTH, WIDTH, WIDTH // 4]
    plan = chunk_plan(row_counts, 4)
    chunks, rows, views = len(plan), RING, 2 * VIEW_ROWS
    any_spec, vmem_spec = pl.BlockSpec(memory_space=pl.ANY), pl.BlockSpec(memory_space=pltpu.VMEM)
    f32, bf16, dma = jnp.float32, jnp.bfloat16, pltpu.SemaphoreType.DMA
    half = WIDTH // 2
    stat = [pltpu.VMEM((4, WIDTH), f32), pltpu.VMEM((4, half), f32), pltpu.VMEM((4, 4, half), f32), pltpu.VMEM((4, 4, half), f32), dma((8,)), dma((8,))]
    scratch = [
        pltpu.VMEM((rows, WIDTH), f32), pltpu.VMEM((rows, WIDTH), f32), pltpu.VMEM((rows, WIDTH // 2), f32),
        pltpu.VMEM((rows, 3 * WIDTH // 8), f32), pltpu.VMEM((rows, 3 * WIDTH // 16), f32),
        dma((chunks, 4, 10)), dma((chunks, 4, 10)), dma((chunks, 2)), dma((chunks, 2)), dma((chunks, 5)),
        pltpu.VMEM((views, WIDTH), bf16), pltpu.VMEM((views, WIDTH), f32), pltpu.VMEM((2, TILE, WIDTH), bf16), pltpu.VMEM((2, views, TILE), f32),
        pltpu.VMEM((2, views, TILE), bf16), pltpu.VMEM((2, TILE, WIDTH), f32),
        *stat, *stat, dma, dma((2,)), dma((2,)), dma((2,)), dma((2,)),
    ]
    shape = jax.ShapeDtypeStruct
    return pl.pallas_call(
        functools.partial(reduce_kernel, row_counts, plan, None, functools.partial(backward_work, num_rows)),
        out_shape=[shape((r, WIDTH), f32) for r in row_counts + row_counts] + [shape((4, WIDTH), f32)] * 2,
        in_specs=[any_spec] * 8 + [vmem_spec], out_specs=[any_spec] * 6 + [vmem_spec] * 2, scratch_shapes=scratch,
        compiler_params=pltpu.CompilerParams(collective_id=collective_id, has_side_effects=True, vmem_limit_bytes=62 * 1024 * 1024),
    )(*work_inputs)


def total_stats(first, second, collective_id):
    local = jnp.concatenate([first, second])
    return sum_stats(local, collective_id).reshape(2, 2, WIDTH)


def batch_norm(pre_act, num_rows):
    totals = total_stats(jnp.sum(pre_act, axis=1), jnp.sum(pre_act * pre_act, axis=1), 0) / num_rows
    inv_std = lax.rsqrt(totals[1] - totals[0] * totals[0] + BN_EPS)
    return (pre_act - totals[0][:, None, :]) * inv_std[:, None, :], totals[0], inv_std


def run_layer(hidden, weight, gain_vec, shift_vec, num_rows):
    pre_act = jnp.einsum('vnf,fd->vnd', hidden, weight, preferred_element_type=jnp.float32)
    normed, mean, inv_std = batch_norm(pre_act, num_rows)
    post_affine = gain_vec * normed + shift_vec
    return jnp.maximum(post_affine, 0.0).astype(jnp.bfloat16), pre_act, jnp.concatenate([gain_vec[None], shift_vec[None], inv_std, mean])


def device_step(num_dev, feat_a, feat_b, w_first, w_second, w_third, gain_first, shift_first, gain_second, shift_second, lam_off):
    num_rows = feat_a.shape[0] * num_dev
    both_views = jnp.stack([feat_a, feat_b])
    hid_one, pre_one, vec_one = run_layer(both_views, w_first, gain_first, shift_first, num_rows)
    hid_two, pre_two, vec_two = run_layer(hid_one, w_second, gain_second, shift_second, num_rows)
    proj_out = jnp.einsum('vnf,fd->vnd', hid_two, w_third, preferred_element_type=jnp.float32)
    emb_norm, _, inv_three = batch_norm(proj_out, num_rows)
    inv_three = inv_three[:, None, :]
    emb_bf = emb_norm.astype(jnp.bfloat16)
    corr_part = lax.dot_general(emb_bf[0], emb_bf[1], (((0,), (0,)), ((), ())), preferred_element_type=jnp.float32)
    grad_corr, loss_part = reduce_all([corr_part], 2, lam_off, num_rows)
    grad_emb_a = lax.dot_general(emb_bf[1], grad_corr, (((1,), (1,)), ((), ())), preferred_element_type=jnp.float32)
    grad_emb_b = jnp.dot(emb_bf[0], grad_corr, preferred_element_type=jnp.float32)
    grad_emb = jnp.stack([grad_emb_a, grad_emb_b]) / num_rows
    local = jnp.concatenate([jnp.sum(grad_emb, axis=1), jnp.sum(grad_emb * emb_norm, axis=1)])
    extra = jnp.full((4, 256), jnp.sum(loss_part), jnp.float32)
    totals = sum_stats(jnp.concatenate([local, extra], axis=1), 1)
    total_loss = totals[0, WIDTH]
    totals = totals[:, :WIDTH].reshape(2, 2, WIDTH) / num_rows
    grad_proj = (inv_three * (grad_emb - totals[0][:, None, :] - emb_norm * totals[1][:, None, :])).astype(jnp.bfloat16)
    flat = lambda t: t.reshape(-1, t.shape[-1])
    grad_third, grad_second, grad_first, _, _, _, total_two, total_one = reduce_with_backward(
        [flat(grad_proj), flat(hid_two), w_third, w_second, flat(pre_two), flat(pre_one), flat(hid_one), flat(both_views), jnp.concatenate([vec_two, vec_one])],
        3, num_rows)
    grad_gain_second, grad_shift_second = total_two[0] + total_two[1], total_two[2] + total_two[3]
    grad_gain_first, grad_shift_first = total_one[0] + total_one[1], total_one[2] + total_one[3]
    return (total_loss, grad_first, grad_second, grad_third, grad_gain_first, grad_shift_first, grad_gain_second, grad_shift_second)


def solution(mesh):
    num_dev = mesh.shape['pod'] * mesh.shape['data']
    row_spec = P(ROW_AXES, None)
    repl_spec = P()
    return jax.shard_map(functools.partial(device_step, num_dev), mesh=mesh, in_specs=(row_spec, row_spec, repl_spec, repl_spec, repl_spec, repl_spec, repl_spec, repl_spec, repl_spec, repl_spec), out_specs=(repl_spec, repl_spec, repl_spec, repl_spec, repl_spec, repl_spec, repl_spec, repl_spec), check_vma=False)
```

```python
import functools
import jax
import jax.numpy as jnp
from jax import lax
from jax.experimental import pallas as pl
from jax.experimental.pallas import tpu as pltpu
from jax.sharding import PartitionSpec as P

BN_EPS = 1e-5
ROW_AXES = ('pod', 'data')
MESH = pl.DeviceIdType.MESH
WIDTH = 2048
QCOLS = WIDTH // 4
CHUNK = 128
BLOCK = CHUNK // 2


def coordinates():
    pod, dat = lax.axis_index('pod'), lax.axis_index('data')
    return lax.div(pod, 2), lax.rem(pod, 2), lax.div(dat, 2), lax.rem(dat, 2)


def device(z, y, x, c):
    return (z * 2 + y, x * 2 + c)


def remote(src, dst, send, recv, dev):
    copy = pltpu.make_async_remote_copy(src_ref=src, dst_ref=dst, send_sem=send, recv_sem=recv, device_id=dev, device_id_type=MESH)
    copy.start()
    return copy


def meet(peers):
    barrier = pltpu.get_barrier_semaphore()
    for dev in peers:
        pl.semaphore_signal(barrier, inc=1, device_id=dev, device_id_type=MESH)
    pl.semaphore_wait(barrier, len(peers))


class StatSum:
    def __init__(self, half, v_ref, o_ref, from_core, plane, line, send, recv):
        z, y, x, c = coordinates()
        self.core_peer = device(z, y, x, 1 - c)
        self.plane_peers = [device(z, y, 1 - x, c), device(z, 1 - y, x, c), device(z, 1 - y, 1 - x, c)]
        self.line_peers = [device(lax.rem(z + o, 4), y, x, c) for o in (1, 2, 3)]
        self.mine = pl.ds(pl.multiple_of(c * half, 128), half)
        self.theirs = pl.ds(pl.multiple_of((1 - c) * half, 128), half)
        self.spot, self.z = y * 2 + x, z
        self.refs, self.sems, self.copies = (v_ref, o_ref, from_core, plane, line), (send, recv), []

    def peers(self):
        return [self.core_peer] + self.plane_peers + self.line_peers

    def send(self, src, dst, devs):
        for dev in devs:
            i = len(self.copies)
            self.copies.append(remote(src, dst, self.sems[0].at[i], self.sems[1].at[i], dev))

    def arrived(self, first, last):
        for copy in self.copies[first:last]:
            copy.wait_recv()

    def step(self, i):
        v_ref, o_ref, from_core, plane, line = self.refs
        if i == 0:
            self.send(v_ref.at[:, self.theirs], from_core, [self.core_peer])
        elif i == 1:
            self.arrived(0, 1)
            plane[self.spot] = v_ref[:, self.mine] + from_core[...]
            self.send(plane.at[self.spot], plane.at[self.spot], self.plane_peers)
        elif i == 2:
            self.arrived(1, 4)
            line[self.z] = (plane[0] + plane[1]) + (plane[2] + plane[3])
            self.send(line.at[self.z], line.at[self.z], self.line_peers)
        elif i == 3:
            self.arrived(4, 7)
            o_ref[:, self.mine] = (line[0] + line[1]) + (line[2] + line[3])
            self.send(o_ref.at[:, self.mine], o_ref.at[:, self.mine], [self.core_peer])
        else:
            self.arrived(7, 8)
            for copy in self.copies:
                copy.wait_send()


def stat_kernel(half, *refs):
    total = StatSum(half, *refs)
    meet(total.peers())
    for i in range(5):
        total.step(i)


def sum_stats(values, collective_id):
    rows, width = values.shape
    half = width // 2
    return pl.pallas_call(
        functools.partial(stat_kernel, half),
        out_shape=jax.ShapeDtypeStruct((rows, width), jnp.float32),
        in_specs=[pl.BlockSpec(memory_space=pltpu.VMEM)],
        out_specs=pl.BlockSpec(memory_space=pltpu.VMEM),
        scratch_shapes=[pltpu.VMEM((rows, half), jnp.float32), pltpu.VMEM((4, rows, half), jnp.float32), pltpu.VMEM((4, rows, half), jnp.float32),
                        pltpu.SemaphoreType.DMA((8,)), pltpu.SemaphoreType.DMA((8,))],
        compiler_params=pltpu.CompilerParams(collective_id=collective_id, has_side_effects=True),
    )(values)


TAPER = (32, 64, 96)
RING = 1024
ORDERS = (('x', 'y', 'z'), ('y', 'x', 'z'), ('x', 'z', 'y'), ('y', 'z', 'x'))
SHARES = {4: {128: (40, 40, 24, 24)}, 2: {128: (48, 48, 16, 16), 96: (32, 32, 16, 16), 64: (32, 32, 0, 0), 32: (16, 16, 0, 0)}}
MIXED = (1,)


def chunk_plan(row_counts, itemsize):
    plan, base = [], 0
    for a, rows in enumerate(row_counts):
        left = rows // 2
        head = [] if a else list(TAPER) if len(row_counts) == 1 else [64]
        tail = list(TAPER[::-1]) if a == len(row_counts) - 1 else []
        left -= sum(head) + sum(tail)
        row = 0
        for size in head + [CHUNK] * (left // CHUNK) + ([left % CHUNK] if left % CHUNK else []) + tail:
            two = (size // 2, size // 2, 0, 0)
            mixed = len(row_counts) == 1 or a in MIXED
            plan.append((a, row, base % RING, size, SHARES[itemsize].get(size, two) if mixed else two))
            row, base = row + size, base + size
    return plan


def reduce_kernel(row_counts, plan, num_rows, work, *refs):
    count = len(row_counts)
    make_grad = num_rows is not None
    if work:
        extra, refs = refs[:WORK_INPUTS], refs[WORK_INPUTS:]
    else:
        parts, refs = refs[:count], refs[count:]
    if make_grad:
        lam_ref, refs = refs[0], refs[1:]
    outs, refs = refs[:count], refs[count:]
    if work:
        parts, extra, refs = refs[:count], extra + refs[:WORK_OUTPUTS], refs[WORK_OUTPUTS:]
    if make_grad:
        loss_ref, refs = refs[0], refs[1:]
    own, from_core, recv_first, recv_second, recv_third, send, recv, core_send, core_recv, local_sem = refs[:10]
    if make_grad:
        shard = refs[10]
        loss_ref[...] = jnp.zeros_like(loss_ref)
    z, y, x, c = coordinates()
    core_peer = device(z, y, x, 1 - c)
    flat_peer = {'x': device(z, y, 1 - x, c), 'y': device(z, 1 - y, x, c)}
    flat_pos = {'x': x, 'y': y}
    line_peers = [device(lax.rem(z + o, 4), y, x, c) for o in (1, 2, 3)]
    plane_peers = [flat_peer['x'], flat_peer['y'], device(z, 1 - y, 1 - x, c)]
    meet([core_peer] + (plane_peers if work else plane_peers[:2]) + line_peers)
    hooks = work(extra + refs[10:]) if work else {}
    chunks = len(plan)
    sends = {}
    parts_of = lambda k: [j for j in range(4) if plan[k][4][j]]
    align = 16 if make_grad else 8
    state = {}

    def start(k):
        a, row, base, size, shares = plan[k]
        sends[k] = []
        for old in list(sends):
            if old < k and plan[old][2] < base + size and base < plan[old][2] + plan[old][3]:
                finish(old)
        half = row_counts[a] // 2
        mine = pl.ds(pl.multiple_of(c * half + row, 16), size)
        theirs = pl.ds(pl.multiple_of((1 - c) * half + row, 16), size)
        load = pltpu.make_async_copy(parts[a].at[mine], own.at[pl.ds(base, size)], local_sem.at[k, 4])
        load.start()
        copy = remote(parts[a].at[theirs], from_core.at[pl.ds(base, size)], core_send.at[k, 0], core_recv.at[k, 0], core_peer)
        sends[k].append(copy)
        state[k] = {'load': load, 'core': copy}
        for j in parts_of(k):
            skip = sum(shares[:j])
            state[k, j] = dict(rows=pl.ds(base + skip, shares[j]), out=row + skip, size=shares[j], col=0, cols=WIDTH)

    def finish(k):
        state[k]['pair'].wait_recv()
        for copy in sends.pop(k):
            copy.wait_send()

    def columns(s):
        return pl.ds(s['col'] if isinstance(s['col'], int) else pl.multiple_of(s['col'], 128), s['cols'])

    def at(s):
        return s['rows'], columns(s)

    def scatter(k, j, step):
        dims = ORDERS[j]
        dim = dims[step]
        s = state[k, j]
        base = 0 if step == 0 else (1 if step == 1 else 2 if dims[1] != 'z' else 4)
        buffer = (recv_first, recv_second, recv_third)[step]
        cols = s['cols'] // (4 if dim == 'z' else 2)
        copies, lands = [], []
        spots = [(lax.rem(z + o, 4), line_peers[o - 1]) for o in (1, 2, 3)] if dim == 'z' else [(1 - flat_pos[dim], flat_peer[dim])]
        for i, (spot, dev) in enumerate(spots):
            land = buffer.at[s['rows'], pl.ds(i * cols, cols)]
            part = dict(s, col=s['col'] + spot * cols, cols=cols)
            copies.append(remote(own.at[at(part)], land, send.at[k, j, base + i], recv.at[k, j, base + i], dev))
            lands.append(land)
        s.update(col=s['col'] + (z if dim == 'z' else flat_pos[dim]) * cols, cols=cols, copies=copies, lands=lands)
        sends[k].extend(copies)

    def absorb(k, j):
        s = state[k, j]
        for copy in s['copies']:
            copy.wait_recv()
        lands = [land[...] for land in s['lands']]
        total = own[at(s)] + lands[0]
        if len(lands) == 3:
            total = total + (lands[1] + lands[2])
        return total

    def first(k):
        _, _, base, size, _ = plan[k]
        state[k]['load'].wait()
        state[k]['core'].wait_recv()
        rows = pl.ds(base, size)
        own[rows] = own[rows] + from_core[rows]
        for j in parts_of(k):
            scatter(k, j, 0)

    def middle(step, k):
        for j in parts_of(k):
            own[at(state[k, j])] = absorb(k, j)
            scatter(k, j, step)

    def out_at(k, s):
        a = plan[k][0]
        row = c * (row_counts[a] // 2) + s['out']
        return outs[a].at[pl.ds(pl.multiple_of(row, align), s['size']), columns(s)]

    def gather(k, j, step):
        dims = ORDERS[j]
        dim = dims[2 - step]
        s = state[k, j]
        base = 5 + (0 if step == 0 else 4 if step == 2 else (1 if dims[2] != 'z' else 3))
        src = out_at(k, s) if step else s['src']
        dst = out_at(k, s)
        peers = line_peers if dim == 'z' else [flat_peer[dim]]
        copies = [remote(src, dst, send.at[k, j, base + i], recv.at[k, j, base + i], dev) for i, dev in enumerate(peers)]
        s.update(col=s['col'] - (z if dim == 'z' else flat_pos[dim]) * s['cols'], cols=(4 if dim == 'z' else 2) * s['cols'], copies=copies)
        if step == 2:
            s.update(col=0)
        sends[k].extend(copies)

    def turn(k):
        a = plan[k][0]
        for j in parts_of(k):
            s = state[k, j]
            total = absorb(k, j)
            if make_grad:
                lam = lam_ref[0, 0]
                corr = total * (1.0 / num_rows)
                row = c * (row_counts[a] // 2) + s['out'] + lax.broadcasted_iota(jnp.int32, corr.shape, 0)
                col = s['col'] + lax.broadcasted_iota(jnp.int32, corr.shape, 1)
                diag = row == col
                miss = 1.0 - corr
                loss = jnp.where(diag, miss * miss, lam * (corr * corr))
                loss_ref[...] = loss_ref[...] + jnp.sum(loss.reshape(s['size'] // 8, 8, 128), axis=0)
                shard[s['rows']] = jnp.where(diag, -2.0 * miss, (2.0 * lam) * corr).astype(jnp.bfloat16)
                s['src'] = shard.at[s['rows']]
            else:
                own[at(s)] = total
                s['src'] = own.at[at(s)]
            s['keep'] = pltpu.make_async_copy(s['src'], out_at(k, s), local_sem.at[k, j])
            s['keep'].start()
            gather(k, j, 0)

    def spread(step, k):
        for j in parts_of(k):
            s = state[k, j]
            for copy in s['copies']:
                copy.wait_recv()
            if step == 1:
                s['keep'].wait()
            gather(k, j, step)

    def pair(k):
        a, row, _, size, _ = plan[k]
        for j in parts_of(k):
            for copy in state[k, j]['copies']:
                copy.wait_recv()
        rows = pl.ds(pl.multiple_of(c * (row_counts[a] // 2) + row, 16), size)
        copy = remote(outs[a].at[rows], outs[a].at[rows], core_send.at[k, 1], core_recv.at[k, 1], core_peer)
        sends[k].append(copy)
        state[k]['pair'] = copy

    stages = [first, functools.partial(middle, 1), functools.partial(middle, 2), turn, functools.partial(spread, 1), functools.partial(spread, 2), pair]
    for t in range(chunks + len(stages) - 1):
        for task in hooks.get(-1, ()) if t == 0 else ():
            task()
        for k in range(chunks):
            if t == (k - 1 if work and k else 0):
                start(k)
        for i, stage in enumerate(stages):
            if 0 <= t - i < chunks:
                stage(t - i)
            if i == 2:
                for task in hooks.get(t, ()):
                    task()
    for k in list(sends):
        finish(k)


def reduce_all(parts, collective_id, lam=None, num_rows=None):
    row_counts = [p.shape[0] for p in parts]
    plan = chunk_plan(row_counts, 2 if lam is not None else 4)
    chunks, rows = len(plan), sum(row_counts) // 2
    any_spec = pl.BlockSpec(memory_space=pl.ANY)
    make_grad = lam is not None
    out_type = jnp.bfloat16 if make_grad else jnp.float32
    in_specs = [any_spec] * len(parts)
    out_specs = [any_spec] * len(parts)
    out_shape = [jax.ShapeDtypeStruct(p.shape, out_type) for p in parts]
    args = list(parts)
    if make_grad:
        in_specs.append(pl.BlockSpec(memory_space=pltpu.SMEM))
        args.append(lam.reshape(1, 1))
        out_specs.append(pl.BlockSpec(memory_space=pltpu.VMEM))
        out_shape.append(jax.ShapeDtypeStruct((8, 128), jnp.float32))
    f32 = jnp.float32
    scratch = [
        pltpu.VMEM((rows, WIDTH), f32), pltpu.VMEM((rows, WIDTH), f32), pltpu.VMEM((rows, WIDTH // 2), f32),
        pltpu.VMEM((rows, 3 * WIDTH // 8), f32), pltpu.VMEM((rows, 3 * WIDTH // 16), f32),
        pltpu.SemaphoreType.DMA((chunks, 4, 10)), pltpu.SemaphoreType.DMA((chunks, 4, 10)),
        pltpu.SemaphoreType.DMA((chunks, 2)), pltpu.SemaphoreType.DMA((chunks, 2)), pltpu.SemaphoreType.DMA((chunks, 5)),
    ]
    if make_grad:
        scratch.append(pltpu.VMEM((rows, WIDTH // 16), jnp.bfloat16))
    return pl.pallas_call(
        functools.partial(reduce_kernel, row_counts, plan, num_rows if make_grad else None, None),
        out_shape=out_shape, in_specs=in_specs, out_specs=out_specs, scratch_shapes=scratch,
        compiler_params=pltpu.CompilerParams(collective_id=collective_id, has_side_effects=True, vmem_limit_bytes=56 * 1024 * 1024),
    )(*args)


WORK_INPUTS, WORK_OUTPUTS = 9, 5
TILE = 256
VIEW_ROWS = 512


def backward_work(num_rows, refs):
    grad_proj, hid_two, w_third, w_second, pre_two, pre_one, hid_one, feats, vec = refs[:9]
    part_third, part_second, part_first, total_two, total_one = refs[9:14]
    grad, act, w_buf, n_buf, x_buf, o_buf = refs[14:20]
    stat_two, stat_one = refs[20:26], refs[26:32]
    grad_sem, w_sem, n_sem, x_sem, o_sem = refs[32:37]
    rows_of = [pl.ds(v * VIEW_ROWS, VIEW_ROWS) for v in range(2)]
    sums = [StatSum(WIDTH // 2, st[0], tot, *st[1:]) for st, tot in ((stat_two, total_two), (stat_one, total_one))]

    def tile(i):
        return pl.ds(pl.multiple_of(i * TILE, TILE), TILE)

    def loop(first, last, fetch, body):
        for copy in fetch(first, first % 2):
            copy.start()

        def trip(i, carry):
            slot = lax.rem(i, 2)

            @pl.when(i + 1 < last)
            def _():
                for copy in fetch(i + 1, 1 - slot):
                    copy.start()
            for copy in fetch(i, slot):
                copy.wait()
            body(i, slot)
            return carry
        lax.fori_loop(first, last, trip, 0)

    def pre_copy(pre, i, slot):
        return pltpu.make_async_copy(pre.at[:, tile(i)], n_buf.at[slot], n_sem.at[slot])

    def normed(slot, v, first, cols):
        return (n_buf[slot, rows_of[v]] - vec[pl.ds(first + 4 + v, 1), cols]) * vec[pl.ds(first + 2 + v, 1), cols]

    def input_grad(layer, first, last):
        weight, pre = ((w_second, pre_one), (w_third, pre_two))[layer]
        stat = (stat_one, stat_two)[layer][0]
        g = 6 if layer == 0 else 0

        def fetch(i, slot):
            return [pltpu.make_async_copy(weight.at[tile(i)], w_buf.at[slot], w_sem.at[slot]), pre_copy(pre, i, slot)]

        def body(i, slot):
            cols = tile(i)
            for v in range(2):
                dx = lax.dot_general(grad[rows_of[v]], w_buf[slot], (((1,), (1,)), ((), ())), preferred_element_type=jnp.float32)
                n = normed(slot, v, g, cols)
                da = jnp.where(vec[pl.ds(g, 1), cols] * n + vec[pl.ds(g + 1, 1), cols] > 0, dx, 0.0)
                act[rows_of[v], cols] = da
                stat[pl.ds(v, 1), cols] = jnp.sum(da * n, axis=0, keepdims=True)
                stat[pl.ds(2 + v, 1), cols] = jnp.sum(da, axis=0, keepdims=True)
        loop(first, last, fetch, body)

    def norm_grad(layer):
        pre, total = ((pre_one, total_one), (pre_two, total_two))[layer]
        g = 6 if layer == 0 else 0

        def body(i, slot):
            cols = tile(i)
            for v in range(2):
                cross = total[pl.ds(v, 1), cols] * (1.0 / num_rows)
                mean = total[pl.ds(2 + v, 1), cols] * (1.0 / num_rows)
                scale = vec[pl.ds(g, 1), cols] * vec[pl.ds(g + 2 + v, 1), cols]
                grad[rows_of[v], cols] = (scale * (act[rows_of[v], cols] - mean - normed(slot, v, g, cols) * cross)).astype(jnp.bfloat16)
        loop(0, WIDTH // TILE, lambda i, slot: [pre_copy(pre, i, slot)], body)

    def weight_grad(hidden, out, first, last):
        tiles = out.shape[0] // TILE
        spot = lambda i: lax.div(i, 2) + lax.rem(i, 2) * (tiles // 2)

        def fetch(i, slot):
            return [pltpu.make_async_copy(hidden.at[:, tile(spot(i))], x_buf.at[slot], x_sem.at[slot])]

        def put(i, slot):
            return pltpu.make_async_copy(o_buf.at[slot], out.at[tile(spot(i))], o_sem.at[slot])

        def body(i, slot):
            @pl.when(i >= first + 2)
            def _():
                put(i, slot).wait()
            for n in range(4):
                cols = pl.ds(n * (WIDTH // 4), WIDTH // 4)
                o_buf[slot, :, cols] = lax.dot_general(x_buf[slot], grad[:, cols], (((0,), (0,)), ((), ())), preferred_element_type=jnp.float32)
            put(i, slot).start()
        loop(first, last, fetch, body)
        for i in (last - 2, last - 1):
            put(i, i % 2).wait()

    grad_load = pltpu.make_async_copy(grad_proj, grad, grad_sem)
    grad_load.start()
    step = lambda which, i: functools.partial(sums[which].step, i)
    run = functools.partial
    return {
        -1: [grad_load.wait, run(weight_grad, hid_two, part_third, 0, 2)], 0: [run(weight_grad, hid_two, part_third, 2, 4)],
        1: [run(weight_grad, hid_two, part_third, 4, 8)], 2: [run(input_grad, 1, 0, 4)], 3: [run(input_grad, 1, 4, 8), step(0, 0)],
        4: [step(0, 1)], 5: [step(0, 2)], 6: [step(0, 3)], 7: [step(0, 4), run(norm_grad, 1), run(weight_grad, hid_one, part_second, 0, 2)],
        8: [run(weight_grad, hid_one, part_second, 2, 8)],
        9: [run(input_grad, 0, 0, 4)], 10: [run(input_grad, 0, 4, 8), step(1, 0)],
        11: [step(1, 1)], 12: [step(1, 2)], 13: [step(1, 3)], 14: [step(1, 4), run(norm_grad, 0)], 15: [run(weight_grad, feats, part_first, 0, 2)],
    }


def reduce_with_backward(work_inputs, collective_id, num_rows):
    row_counts = [WIDTH, WIDTH, WIDTH // 4]
    plan = chunk_plan(row_counts, 4)
    chunks, rows, views = len(plan), RING, 2 * VIEW_ROWS
    any_spec, vmem_spec = pl.BlockSpec(memory_space=pl.ANY), pl.BlockSpec(memory_space=pltpu.VMEM)
    f32, bf16, dma = jnp.float32, jnp.bfloat16, pltpu.SemaphoreType.DMA
    half = WIDTH // 2
    stat = [pltpu.VMEM((4, WIDTH), f32), pltpu.VMEM((4, half), f32), pltpu.VMEM((4, 4, half), f32), pltpu.VMEM((4, 4, half), f32), dma((8,)), dma((8,))]
    scratch = [
        pltpu.VMEM((rows, WIDTH), f32), pltpu.VMEM((rows, WIDTH), f32), pltpu.VMEM((rows, WIDTH // 2), f32),
        pltpu.VMEM((rows, 3 * WIDTH // 8), f32), pltpu.VMEM((rows, 3 * WIDTH // 16), f32),
        dma((chunks, 4, 10)), dma((chunks, 4, 10)), dma((chunks, 2)), dma((chunks, 2)), dma((chunks, 5)),
        pltpu.VMEM((views, WIDTH), bf16), pltpu.VMEM((views, WIDTH), f32), pltpu.VMEM((2, TILE, WIDTH), bf16), pltpu.VMEM((2, views, TILE), f32),
        pltpu.VMEM((2, views, TILE), bf16), pltpu.VMEM((2, TILE, WIDTH), f32),
        *stat, *stat, dma, dma((2,)), dma((2,)), dma((2,)), dma((2,)),
    ]
    shape = jax.ShapeDtypeStruct
    return pl.pallas_call(
        functools.partial(reduce_kernel, row_counts, plan, None, functools.partial(backward_work, num_rows)),
        out_shape=[shape((r, WIDTH), f32) for r in row_counts + row_counts] + [shape((4, WIDTH), f32)] * 2,
        in_specs=[any_spec] * 8 + [vmem_spec], out_specs=[any_spec] * 6 + [vmem_spec] * 2, scratch_shapes=scratch,
        compiler_params=pltpu.CompilerParams(collective_id=collective_id, has_side_effects=True, vmem_limit_bytes=62 * 1024 * 1024),
    )(*work_inputs)


def total_stats(first, second, collective_id):
    local = jnp.concatenate([first, second])
    return sum_stats(local, collective_id).reshape(2, 2, WIDTH)


def batch_norm(pre_act, num_rows):
    totals = total_stats(jnp.sum(pre_act, axis=1), jnp.sum(pre_act * pre_act, axis=1), 0) / num_rows
    inv_std = lax.rsqrt(totals[1] - totals[0] * totals[0] + BN_EPS)
    return (pre_act - totals[0][:, None, :]) * inv_std[:, None, :], totals[0], inv_std


def run_layer(hidden, weight, gain_vec, shift_vec, num_rows):
    pre_act = jnp.einsum('vnf,fd->vnd', hidden, weight, preferred_element_type=jnp.float32)
    normed, mean, inv_std = batch_norm(pre_act, num_rows)
    post_affine = gain_vec * normed + shift_vec
    return jnp.maximum(post_affine, 0.0).astype(jnp.bfloat16), pre_act, jnp.concatenate([gain_vec[None], shift_vec[None], inv_std, mean])


def device_step(num_dev, feat_a, feat_b, w_first, w_second, w_third, gain_first, shift_first, gain_second, shift_second, lam_off):
    num_rows = feat_a.shape[0] * num_dev
    both_views = jnp.stack([feat_a, feat_b])
    hid_one, pre_one, vec_one = run_layer(both_views, w_first, gain_first, shift_first, num_rows)
    hid_two, pre_two, vec_two = run_layer(hid_one, w_second, gain_second, shift_second, num_rows)
    proj_out = jnp.einsum('vnf,fd->vnd', hid_two, w_third, preferred_element_type=jnp.float32)
    emb_norm, _, inv_three = batch_norm(proj_out, num_rows)
    inv_three = inv_three[:, None, :]
    emb_bf = emb_norm.astype(jnp.bfloat16)
    corr_part = lax.dot_general(emb_bf[0], emb_bf[1], (((0,), (0,)), ((), ())), preferred_element_type=jnp.float32)
    grad_corr, loss_part = reduce_all([corr_part], 2, lam_off, num_rows)
    grad_emb_a = lax.dot_general(emb_bf[1], grad_corr, (((1,), (1,)), ((), ())), preferred_element_type=jnp.float32)
    grad_emb_b = jnp.dot(emb_bf[0], grad_corr, preferred_element_type=jnp.float32)
    grad_emb = jnp.stack([grad_emb_a, grad_emb_b]) / num_rows
    local = jnp.concatenate([jnp.sum(grad_emb, axis=1), jnp.sum(grad_emb * emb_norm, axis=1)])
    extra = jnp.full((4, 256), jnp.sum(loss_part), jnp.float32)
    totals = sum_stats(jnp.concatenate([local, extra], axis=1), 1)
    total_loss = totals[0, WIDTH]
    totals = totals[:, :WIDTH].reshape(2, 2, WIDTH) / num_rows
    grad_proj = (inv_three * (grad_emb - totals[0][:, None, :] - emb_norm * totals[1][:, None, :])).astype(jnp.bfloat16)
    flat = lambda t: t.reshape(-1, t.shape[-1])
    grad_third, grad_second, grad_first, _, _, _, total_two, total_one = reduce_with_backward(
        [flat(grad_proj), flat(hid_two), w_third, w_second, flat(pre_two), flat(pre_one), flat(hid_one), flat(both_views), jnp.concatenate([vec_two, vec_one])],
        3, num_rows)
    grad_gain_second, grad_shift_second = total_two[0] + total_two[1], total_two[2] + total_two[3]
    grad_gain_first, grad_shift_first = total_one[0] + total_one[1], total_one[2] + total_one[3]
    return (total_loss, grad_first, grad_second, grad_third, grad_gain_first, grad_shift_first, grad_gain_second, grad_shift_second)


def solution(mesh):
    num_dev = mesh.shape['pod'] * mesh.shape['data']
    row_spec = P(ROW_AXES, None)
    repl_spec = P()
    return jax.shard_map(functools.partial(device_step, num_dev), mesh=mesh, in_specs=(row_spec, row_spec, repl_spec, repl_spec, repl_spec, repl_spec, repl_spec, repl_spec, repl_spec, repl_spec), out_specs=(repl_spec, repl_spec, repl_spec, repl_spec, repl_spec, repl_spec, repl_spec, repl_spec), check_vma=False)
```
